256 devices in a mesh: seq: 8 (over x, y_hi), head: 32 (over z, y_lo, core).
Axes of the slice: x: 4, y: 4 (y_hi: 2, y_lo: 2; y = y_hi * 2 + y_lo), z: 8, core: 2. Of those that a mesh axis runs over, the one named last changes fastest.
Arguments:
- xraw: bfloat16 [8192, 8192], P('seq', 'head'), may hold values from -6 to 6
- zgate: bfloat16 [8192, 8192], P('seq', 'head'), may hold values from -6 to 6
- bcraw: bfloat16 [8192, 256], P('seq'), may hold values from -6 to 6
- dt: float32 [128, 8192], P('head', 'seq'), may hold values from 3.0517578e-06 to 0.25, as said below
- a_rate: float32 [128], P('head'), may hold values from 1 to 2
- d_skip: float32 [128], P('head'), may hold values from 0.5 to 1.5
- conv_x: float32 [4, 8192], P(None, 'head'), may hold values from -3 to 3
- conv_bc: float32 [4, 256], replicated, may hold values from -3 to 3
- dout: bfloat16 [8192, 8192], P('seq', 'head'), may hold values from -6 to 6
Outputs:
- x_raw_grad: bfloat16 [8192, 8192], P('seq', 'head')
- gate_grad: bfloat16 [8192, 8192], P('seq', 'head')
- step_grad: float32 [128, 8192], P('head', 'seq')
- bc_raw_grad: float32 [8192, 256], P(('seq', 'head'))
- conv_x_grad: float32 [4, 8192], P(None, 'head')
- conv_bc_grad: float32 [4, 256], replicated
The draws below stay inside these ranges and needn't reach their ends.
Inputs may be any that keep to these rules, and one draw needn't show every extreme that they name: `dt`: positive step sizes.
All inputs are finite; a program needn't handle non-finite values.
Results may differ from the reference program's by a relative error of at most 0.028.
Values may be sent and summed in bfloat16 or wider, within the bound.
A program may use at most 64 MiB of HBM per device.

```python
import math
import jax
import jax.numpy as jnp
from jax import lax

HEADS = 128
HEAD_DIM = 64
STATE = 128
GROUP = 256
CONV = 4
TOKEN_COUNT = 8192


def draw_dt(key, part):
    quick_random_key, random_base_key, jagged_random_key, spike_random_key = jax.random.split(key, 4)
    fast_share = 0.5
    fast_heads = jax.random.uniform(quick_random_key, (HEADS,)) < fast_share
    levels = jax.random.uniform(random_base_key, (HEADS,))
    slow_rate = jnp.exp(jnp.log(0.05) + levels * (jnp.log(0.3) - jnp.log(0.05))) / TOKEN_COUNT
    fast_rate = jnp.exp(jnp.log(1.0 / 60.0) + levels * (jnp.log(1.0 / 25.0) - jnp.log(1.0 / 60.0)))
    base_rate = jnp.where(fast_heads, fast_rate, slow_rate)
    roughness = jax.random.uniform(jagged_random_key, (HEADS, TOKEN_COUNT), minval=0.5, maxval=1.5)
    step_size_values = base_rate[:, None] * roughness
    spike_positions_list = jax.random.randint(spike_random_key, (3,), 0, TOKEN_COUNT)
    spike_mask = jnp.any(jnp.arange(TOKEN_COUNT, dtype=jnp.int32)[None, :] == spike_positions_list[:, None], axis=0)
    return jnp.where(spike_mask[None, :], 0.25, step_size_values).astype(jnp.float32)


def steps_of(own_key, dims, cuts, low, high):
    def one(axis_at, blocks):
        steps = jax.random.uniform(jax.random.fold_in(jax.random.fold_in(own_key, 6), axis_at), (blocks,), jnp.float32, low / len(cuts), high / len(cuts))
        return jnp.repeat(jnp.exp(steps), dims[axis_at] // blocks).reshape((-1,) + (1,) * (len(dims) - axis_at - 1))

    level = one(*cuts[0])
    for cut in cuts[1:]:
        level = level * one(*cut)
    return level


def scatter_about(stream_key, shape, width, limit, shards=(), kind=jnp.bfloat16):
    entries = width * jax.random.normal(stream_key, shape, jnp.float32)
    if shards:
        entries = entries * steps_of(stream_key, shape, shards, -0.22, 0.18)
    return jnp.clip(entries, -limit, limit).astype(kind)


def setup_inputs(seed: int = 0) -> dict:
    streams_of = jax.random.split(jax.random.key(seed), 10)
    xraw = scatter_about(streams_of[0], (TOKEN_COUNT, HEADS * HEAD_DIM), 1.0, 6.0, ((0, 8), (1, 32)))
    zgate = scatter_about(streams_of[1], (TOKEN_COUNT, HEADS * HEAD_DIM), 1.0, 6.0, ((0, 8), (1, 32)))
    bcraw = scatter_about(streams_of[2], (TOKEN_COUNT, 2 * STATE), 1.0, 6.0, ((0, 8),))
    dt = draw_dt(jax.random.fold_in(streams_of[9], 71), 0)
    a_rate = jnp.clip(jnp.exp(math.log(2.0) - 0.6931472 * jax.random.uniform(streams_of[4], (HEADS,), jnp.float32) ** steps_of(streams_of[4], (HEADS,), ((0, 32),), -0.2, 0.2)), 1.0, 2.0)
    d_skip = jnp.clip(0.5 + 1.0 * jax.random.uniform(streams_of[5], (HEADS,), jnp.float32) ** steps_of(streams_of[5], (HEADS,), ((0, 32),), -0.2, 0.2), 0.5, 1.5)
    conv_x = scatter_about(streams_of[6], (CONV, HEADS * HEAD_DIM), CONV ** -0.5, 3.0, ((1, 32),), jnp.float32)
    conv_bc = scatter_about(streams_of[7], (CONV, 2 * STATE), CONV ** -0.5, 3.0, (), jnp.float32)
    dout = scatter_about(streams_of[8], (TOKEN_COUNT, HEADS * HEAD_DIM), 1.0, 6.0, ((0, 8), (1, 32)))
    return {"xraw": xraw, "zgate": zgate, "bcraw": bcraw, "dt": dt, "a_rate": a_rate, "d_skip": d_skip, "conv_x": conv_x, "conv_bc": conv_bc, "dout": dout}


def silu_slope(values):
    logistic = jax.nn.sigmoid(values)
    return logistic * (1.0 + values * (1.0 - logistic))

def conv_apply(extended, weight, length):
    conv_len = weight.shape[0]
    running = jnp.zeros((length, extended.shape[1]), jnp.float32)
    for offset in range(conv_len):
        start_row = conv_len - 1 - offset
        running = running + weight[offset][None, :] * extended[start_row:start_row + length].astype(jnp.float32)
    return running

def conv_adjoint(extended, weight, length):
    conv_len = weight.shape[0]
    running = jnp.zeros((length, extended.shape[1]), jnp.float32)
    for offset in range(conv_len):
        running = running + weight[offset][None, :] * extended[offset:offset + length]
    return running

def conv_weight_grad(slope_rows, raw_extended, conv_len):
    length = slope_rows.shape[0]
    rows_list = []
    for offset in range(conv_len):
        start_row = conv_len - 1 - offset
        rows_list.append(lax.optimization_barrier(jnp.sum(slope_rows * raw_extended[start_row:start_row + length].astype(jnp.float32), axis=0)))
    return jnp.stack(rows_list)

def pair_decay(within_block):
    block_len = within_block.shape[-1]
    places = jnp.arange(block_len, dtype=jnp.int32)
    causal = (places[:, None] >= places[None, :]).astype(jnp.float32)
    return jnp.exp(jnp.minimum(within_block[..., None, :] - within_block[..., :, None], 0.0)) * causal

def block_tables(b_b, c_b, within_b):
    totals_b = within_b[:, -1]
    decay_b = pair_decay(within_b)
    scores = jnp.dot(c_b, b_b.T, preferred_element_type=jnp.float32)
    kernel = (scores[None] * decay_b).astype(jnp.bfloat16)
    enter = jnp.exp(-within_b).T[:, :, None]
    leave = jnp.exp(-(totals_b[:, None] - within_b)).T[:, :, None]
    return (totals_b, decay_b, kernel, enter, leave)

def reference(xraw, zgate, bcraw, dt, a_rate, d_skip, conv_x, conv_bc, dout):
    length = xraw.shape[0]
    head_count = HEADS
    head_size = HEAD_DIM
    state_dim = STATE
    block_len = GROUP
    block_count = length // block_len
    conv_len = CONV
    x_extended = jnp.pad(xraw, ((conv_len - 1, 0), (0, 0)))
    bc_extended = jnp.pad(bcraw, ((conv_len - 1, 0), (0, 0)))
    x_post = jax.nn.silu(conv_apply(x_extended, conv_x, length)).astype(jnp.bfloat16)
    bc_pre = conv_apply(bc_extended, conv_bc, length)
    bc_post = jax.nn.silu(bc_pre).astype(jnp.bfloat16)
    b_blocks = bc_post[:, :state_dim].reshape(block_count, block_len, state_dim)
    c_blocks = bc_post[:, state_dim:].reshape(block_count, block_len, state_dim)
    x_blocks = x_post.reshape(block_count, block_len, head_count, head_size)
    step_blocks = dt.reshape(head_count, block_count, block_len).transpose(1, 0, 2)
    within = jnp.cumsum(a_rate[None, :, None] * step_blocks, axis=2)
    w_blocks = (x_blocks.astype(jnp.float32) * step_blocks.transpose(0, 2, 1)[..., None]).astype(jnp.bfloat16)
    gate_blocks = zgate.reshape(block_count, block_len, head_count, head_size)
    dout_blocks = dout.reshape(block_count, block_len, head_count, head_size)

    def forward_block(carried, pieces):
        x_b, w_b, b_b, c_b, within_b, gate_b, dout_b = pieces
        totals_b, decay_b, kernel, enter, leave = block_tables(b_b, c_b, within_b)
        states_bf = carried.astype(jnp.bfloat16)
        inner_part = jnp.einsum('hts,shp->thp', kernel.astype(jnp.float32), w_b.astype(jnp.float32))
        outer_part = jnp.einsum('tn,hpn->thp', c_b.astype(jnp.float32), states_bf.astype(jnp.float32)) * enter
        output_y = inner_part + outer_part + d_skip[None, :, None] * x_b.astype(jnp.float32)
        gate_f = gate_b.astype(jnp.float32)
        gate_grad = (dout_b.astype(jnp.float32) * output_y * silu_slope(gate_f)).astype(jnp.bfloat16)
        w_leave = (w_b.astype(jnp.float32) * leave).astype(jnp.bfloat16)
        ends = jnp.einsum('shp,sn->hpn', w_leave.astype(jnp.float32), b_b.astype(jnp.float32))
        carried = jnp.exp(-totals_b)[:, None, None] * carried + ends
        return (carried, (states_bf, gate_grad))
    start_state = jnp.zeros((head_count, head_size, state_dim), jnp.float32)
    unused, (states_all, gate_all) = lax.scan(forward_block, start_state, (x_blocks, w_blocks, b_blocks, c_blocks, within, gate_blocks, dout_blocks))

    def backward_block(carried, pieces):
        x_b, w_b, b_b, c_b, within_b, gate_b, dout_b, step_b, states_bf = pieces
        totals_b, decay_b, kernel, enter, leave = block_tables(b_b, c_b, within_b)
        grads_bf = carried.astype(jnp.bfloat16)
        dy_bf = (dout_b.astype(jnp.float32) * jax.nn.silu(gate_b.astype(jnp.float32))).astype(jnp.bfloat16)
        dy_f = dy_bf.astype(jnp.float32)
        dy_enter = (dy_f * enter).astype(jnp.bfloat16)
        w_f = w_b.astype(jnp.float32)
        w_grad = jnp.einsum('hts,thp->shp', kernel.astype(jnp.float32), dy_f) + leave * jnp.einsum('sn,hpn->shp', b_b.astype(jnp.float32), grads_bf.astype(jnp.float32))
        x_grad = step_b.T[:, :, None] * w_grad + d_skip[None, :, None] * dy_f
        step_grad = lax.optimization_barrier(jnp.sum(x_b.astype(jnp.float32) * w_grad, axis=2))
        mixing = jnp.einsum('thp,shp->hts', dy_f, w_f)
        mixed = lax.optimization_barrier(jnp.sum(mixing * decay_b, axis=0)).astype(jnp.bfloat16)
        c_grad = jnp.dot(mixed, b_b, preferred_element_type=jnp.float32) + lax.optimization_barrier(jnp.sum(enter * jnp.einsum('thp,hpn->thn', dy_f, states_bf.astype(jnp.float32)), axis=1))
        b_grad = jnp.dot(mixed.T, c_b, preferred_element_type=jnp.float32) + lax.optimization_barrier(jnp.sum(leave * jnp.einsum('shp,hpn->shn', w_f, grads_bf.astype(jnp.float32)), axis=1))
        starts_grad = jnp.einsum('thp,tn->hpn', dy_enter.astype(jnp.float32), c_b.astype(jnp.float32))
        carried = jnp.exp(-totals_b)[:, None, None] * carried + starts_grad
        return (carried, (x_grad, step_grad, jnp.concatenate([b_grad, c_grad], axis=-1)))
    unused_grad, (x_grads, step_grads, shared) = lax.scan(backward_block, start_state, (x_blocks, w_blocks, b_blocks, c_blocks, within, gate_blocks, dout_blocks, step_blocks, states_all), reverse=True)
    x_pre = conv_apply(x_extended, conv_x, length)
    x_slope = x_grads.reshape(length, head_count * head_size) * silu_slope(x_pre)
    x_raw_grad = conv_adjoint(jnp.pad(x_slope, ((0, conv_len - 1), (0, 0))), conv_x, length).astype(jnp.bfloat16)
    conv_x_grad = conv_weight_grad(x_slope, x_extended, conv_len)
    bc_slope = shared.reshape(length, 2 * state_dim) * silu_slope(bc_pre)
    bc_raw_grad = conv_adjoint(jnp.pad(bc_slope, ((0, conv_len - 1), (0, 0))), conv_bc, length)
    conv_bc_grad = conv_weight_grad(bc_slope, bc_extended, conv_len)
    step_grad = step_grads.reshape(length, head_count).T
    gate_grad = gate_all.reshape(length, head_count * head_size)
    return (x_raw_grad, gate_grad, step_grad, bc_raw_grad, conv_x_grad, conv_bc_grad)
```

```python
import functools

import jax
import jax.numpy as jnp
from jax import lax
from jax.experimental import pallas as pl
from jax.experimental.pallas import tpu as pltpu
from jax.sharding import Mesh
from jax.sharding import PartitionSpec as P

HEAD_DIM = 64
BLOCK = 256
TAPS = 4
SEQ = ("seq_0", "seq_1")
HEAD = ("head_0", "head_1", "head_2")
SEQ_HEAD = SEQ + HEAD
F32, BF16 = jnp.float32, jnp.bfloat16


def mm(a, b, dims=((1,), (0,))):
    return lax.dot_general(a, b, (dims, ((), ())), preferred_element_type=F32)


NT = ((1,), (1,))
TN = ((0,), (0,))


def parts3(v):
    p1 = v.astype(BF16)
    r1 = v - p1.astype(F32)
    p2 = r1.astype(BF16)
    r2 = r1 - p2.astype(F32)
    return p1, p2, r2.astype(BF16)


def sigmoid(v):
    return 1.0 / (1.0 + jnp.exp(-v))


def by_head(scalars, lanes):
    out = jnp.full(lanes.shape, scalars[3], F32)
    for h in (2, 1, 0):
        out = jnp.where(lanes == h, scalars[h], out)
    return out


def kernel(
    dims, T, W,
    xraw, zg, bcr, dt, a_s, d_s, cvx, cvb, dout,
    xg_o, gg_o, sg_o, bg_o, cx_o, cb_o,
    XF, BCF, XS, BCS, GZ, DTE, ENT, LEA, YIN, WGIN, XSL, BS,
    XP, WX, WL, DY, DYE, BCP, MX,
    GC, DC, WP, TOT, EK, BK, LS, NS, SB, GB, EB, SLOT,
    KH, WXM, DYM, HXR, HBR, HSX, HSB,
    PR, RA, A1S, A1K, RB, A2, ZS, RZ, CXS, CBS, CBL, CBT, CBZ,
    s_h, r_h, s_st, r_st, s_sl, r_sl, s_a, r_a, s_b, r_b, s_z, r_z,
    s_cx, r_cx, s_cb, r_cb, s_cc, r_cc, s_cz, r_cz,
):
    nx, nyh, nz, nyl, nc = dims
    nseq = nx * nyh
    nb = T // BLOCK
    heads = W // HEAD_DIM
    own = T // (nz * nyl * nc)
    sx, sy = lax.axis_index("seq_0"), lax.axis_index("seq_1")
    s = sx * nyh + sy
    z, yl, c = (lax.axis_index(n) for n in HEAD)

    def at_seq(p):
        return {"seq_0": p // nyh, "seq_1": lax.rem(p, nyh)}

    def other(d):
        wrapped = (s + d) // nseq
        return s + d - nseq * wrapped, wrapped

    def other_z(d):
        return lax.rem(z + d, nz)

    def send(src, dst, ss, rs, dev):
        return pltpu.make_async_remote_copy(
            src_ref=src, dst_ref=dst, send_sem=ss, recv_sem=rs,
            device_id=dev, device_id_type=pl.DeviceIdType.MESH,
        )

    core_dev = {"head_2": 1 - c}
    y_dev = {"head_1": 1 - yl}

    barrier = pltpu.get_barrier_semaphore()

    def greet(dev):
        pl.semaphore_signal(barrier, inc=1, device_id=dev, device_id_type=pl.DeviceIdType.MESH)

    for d in range(1, nseq):
        greet(at_seq(other(d)[0]))
    for d in range(1, nz):
        greet({"head_0": other_z(d)})
    greet(core_dev)
    greet(y_dev)

    rows16 = lax.broadcasted_iota(jnp.int32, (heads, BLOCK), 0)
    a_col = by_head([a_s[h] for h in range(heads)], rows16)
    for k in range(nb):
        piece = dt[:, k * BLOCK : (k + 1) * BLOCK]
        DC[k * heads : (k + 1) * heads, :] = piece
        GC[k * heads : (k + 1) * heads, :] = piece * a_col
    n16 = nb * heads
    ri = lax.broadcasted_iota(jnp.int32, (BLOCK, BLOCK), 0)
    ci = lax.broadcasted_iota(jnp.int32, (BLOCK, BLOCK), 1)
    tri = (ri <= ci).astype(F32).astype(BF16)
    w3 = mm(jnp.concatenate(parts3(GC[...]), axis=0), tri)
    within = w3[:n16] + w3[n16 : 2 * n16] + w3[2 * n16 :]
    GC[...] = within
    wp = jnp.concatenate(parts3(within), axis=0)
    dp = jnp.concatenate(parts3(DC[...]), axis=0)
    WP[...] = wp
    rr = lax.rem(lax.broadcasted_iota(jnp.int32, (3 * n16, W), 0), n16)
    ll = lax.broadcasted_iota(jnp.int32, (3 * n16, W), 1) // HEAD_DIM

    def blk(k, n=BLOCK):
        return pl.ds(pl.multiple_of(k * n, n), n)

    def expand(k, carry):
        hot = ((rr // heads == k) & (lax.rem(rr, heads) == ll)).astype(F32).astype(BF16)
        wexp = mm(wp, hot, TN)
        total = wexp[BLOCK - 1 : BLOCK, :]
        TOT[k] = jnp.broadcast_to(total, (8, W))
        ENT[blk(k), :] = jnp.exp(-wexp)
        LEA[blk(k), :] = jnp.exp(jnp.minimum(wexp - total, 0.0))
        DTE[blk(k), :] = mm(dp, hot, TN)
        return carry

    lax.fori_loop(0, nb, expand, 0)

    CH = 64

    def gates(i, carry):
        r = blk(i, CH)
        zv = zg[r, :].astype(F32)
        q = sigmoid(zv)
        up = dout[r, :].astype(F32)
        dy = (up * (zv * q)).astype(BF16)
        DY[r, :] = dy
        GZ[r, :] = up * (q * (1.0 + zv * (1.0 - q)))
        DYE[r, :] = (dy.astype(F32) * ENT[r, :]).astype(BF16)
        shifted = pl.ds(pl.multiple_of(8 + i * CH, 8), CH)
        XF[shifted, :] = xraw[r, :].astype(F32)
        BCF[shifted, :] = bcr[r, :].astype(F32)
        return carry

    lax.fori_loop(0, T // CH, gates, 0)

    pl.semaphore_wait(barrier, nseq - 1 + nz - 1 + 2)

    halo_x = send(xraw.at[T - 16 :], HXR, s_h.at[0], r_h.at[0], at_seq(s + 1))
    halo_b = send(bcr.at[T - 16 :], HBR, s_h.at[1], r_h.at[1], at_seq(s + 1))

    @pl.when(s < nseq - 1)
    def _():
        halo_x.start()
        halo_b.start()

    def conv_chunk(i, carry):
        r = blk(i, CH)
        ext = pl.ds(pl.multiple_of(i * CH, 8), CH + 8)

        def pre(F, taps):
            v = F[ext, :]
            out = taps[0:1, :] * v[8:, :]
            for k in range(1, TAPS):
                out = out + taps[k : k + 1, :] * pltpu.roll(v, k, 0)[8:, :]
            return out

        v = pre(BCF, cvb)
        q = sigmoid(v)
        BCP[r, :] = (v * q).astype(BF16)
        BCS[r, :] = q * (1.0 + v * (1.0 - q))
        v = pre(XF, cvx)
        q = sigmoid(v)
        post = (v * q).astype(BF16)
        XP[r, :] = post
        XS[r, :] = q * (1.0 + v * (1.0 - q))
        wx = (post.astype(F32) * DTE[r, :]).astype(BF16)
        WX[r, :] = wx
        WL[r, :] = (wx.astype(F32) * LEA[r, :]).astype(BF16)
        return carry

    per = BLOCK // CH
    N = W // 2

    def block_ends(k, carry):
        EK[k] = mm(BCP[blk(k), :N], WL[blk(k), :], TN)
        BK[k] = mm(BCP[blk(k), N:], DYE[blk(k), :], TN)
        return carry

    lax.fori_loop(per, nb * per, conv_chunk, 0)
    lax.fori_loop(1, nb, block_ends, 0)

    @pl.when(s > 0)
    def _():
        halo_x.wait_recv()
        halo_b.wait_recv()
        XF[0:8, :] = HXR[8:16, :].astype(F32)
        BCF[0:8, :] = HBR[8:16, :].astype(F32)

    @pl.when(s == 0)
    def _():
        XF[0:8, :] = jnp.zeros((8, W), F32)
        BCF[0:8, :] = jnp.zeros((8, W), F32)

    lax.fori_loop(0, per, conv_chunk, 0)
    block_ends(0, 0)

    state = jnp.zeros((N, W), F32)
    for k in range(nb):
        LS[k] = state
        state = jnp.exp(-TOT[k][0:1, :]) * state + EK[k]
    grad = jnp.zeros((N, W), F32)
    for k in reversed(range(nb)):
        NS[k] = grad
        grad = jnp.exp(-TOT[k][0:1, :]) * grad + BK[k]
    dtot = TOT[0]
    for k in range(1, nb):
        dtot = dtot + TOT[k]
    q1, q2, q3 = (p.astype(F32) for p in parts3(dtot[0:1, :]))
    rt = lax.broadcasted_iota(jnp.int32, (16, W), 0)
    tail = jnp.where(rt == 0, q1, jnp.where(rt == 1, q2, jnp.where(rt == 2, q3, 0.0)))
    tail = tail.astype(BF16)
    EB[0, 0:N, :] = state.astype(BF16)
    EB[1, 0:N, :] = grad.astype(BF16)
    EB[0, N : N + 16, :] = tail
    EB[1, N : N + 16, :] = tail

    def state_copy(d):
        p, wrapped = other(d)
        return send(EB.at[wrapped], SLOT.at[s], s_st.at[d], r_st.at[s], at_seq(p))

    for d in range(1, nseq):
        state_copy(d).start()

    lane_h = lax.broadcasted_iota(jnp.int32, (BLOCK, W), 1) // HEAD_DIM
    r512 = lax.rem(lax.broadcasted_iota(jnp.int32, (3 * n16, heads * 128), 0), n16)
    l512 = lax.broadcasted_iota(jnp.int32, (3 * n16, heads * 128), 1) // 128
    for h in range(heads):
        KH[0:128, h * BLOCK + 128 : (h + 1) * BLOCK] = jnp.zeros((128, 128), BF16)
    TQ = 64

    def inside(k, carry):
        bm, cm = BCP[blk(k), :N], BCP[blk(k), N:]
        wx, dy = WX[blk(k), :], DY[blk(k), :]
        for h in range(heads):
            WXM[h * BLOCK : (h + 1) * BLOCK, :] = jnp.where(lane_h == h, wx, jnp.zeros_like(wx))
            DYM[h * BLOCK : (h + 1) * BLOCK, :] = jnp.where(lane_h == h, dy, jnp.zeros_like(dy))
        hot = ((r512 // heads == k) & (lax.rem(r512, heads) == l512)).astype(F32).astype(BF16)
        col = mm(WP[...], hot, TN)
        for t0 in range(0, BLOCK, TQ):
            ext = 128 if t0 < 128 else BLOCK
            sc = mm(cm[t0 : t0 + TQ, :], bm[0:ext, :], NT)
            tt = t0 + lax.broadcasted_iota(jnp.int32, (TQ, ext), 0)
            ss = lax.broadcasted_iota(jnp.int32, (TQ, ext), 1)
            keep = tt >= ss
            total = None
            for h in range(heads):
                wrow = GC[pl.ds(k * heads + h, 1), :][:, 0:ext]
                wcol = col[t0 : t0 + TQ, h * 128 : (h + 1) * 128]
                if ext > 128:
                    wcol = jnp.concatenate([wcol, wcol], axis=1)
                decay = jnp.where(keep, jnp.exp(jnp.minimum(wrow - wcol, 0.0)), 0.0)
                KH[t0 : t0 + TQ, h * BLOCK : h * BLOCK + ext] = (sc * decay).astype(BF16)
                mixing = mm(DYM[h * BLOCK + t0 : h * BLOCK + t0 + TQ, :], wx[0:ext, :], NT)
                part = mixing * decay
                total = part if total is None else total + part
            rows = pl.ds(pl.multiple_of(k * BLOCK + t0, TQ), TQ)
            MX[rows, 0:ext] = total.astype(BF16)
            if ext < BLOCK:
                MX[rows, ext:] = jnp.zeros((TQ, BLOCK - ext), BF16)
        YIN[blk(k), :] = mm(KH[...], WXM[...])
        acc = None
        for h in range(heads):
            part = mm(KH[:, h * BLOCK : (h + 1) * BLOCK], DYM[h * BLOCK : (h + 1) * BLOCK, :], TN)
            acc = part if acc is None else acc + part
        WGIN[blk(k), :] = acc
        return carry

    lax.fori_loop(0, nb, inside, 0)

    for d in range(1, nseq):
        p, _ = other(d)
        send(EB.at[0], SLOT.at[p], s_st.at[d], r_st.at[p], at_seq(p)).wait_recv()

    def fold(p, value):
        t3 = SLOT[p, N : N + 16, :].astype(F32)
        dec = jnp.exp(-(t3[0:1, :] + t3[1:2, :] + t3[2:3, :]))
        return dec * value + SLOT[p, 0:N, :].astype(F32)

    s_in = lax.fori_loop(0, s, fold, jnp.zeros((N, W), F32))
    g_in = lax.fori_loop(0, nseq - 1 - s, lambda i, v: fold(nseq - 1 - i, v), jnp.zeros((N, W), F32))
    before = jnp.zeros((1, W), F32)
    for k in range(nb):
        SB[k] = (LS[k] + jnp.exp(-before) * s_in).astype(BF16)
        before = before + TOT[k][0:1, :]
    after = jnp.zeros((1, W), F32)
    for k in reversed(range(nb)):
        GB[k] = (NS[k] + jnp.exp(-after) * g_in).astype(BF16)
        after = after + TOT[k][0:1, :]

    def shared(k, carry):
        r = blk(k)
        mx = MX[r, :]
        bg = mm(mx, BCP[r, N:], TN) + mm(WL[r, :], GB[k], NT)
        cg = mm(mx, BCP[r, :N]) + mm(DYE[r, :], SB[k], NT)
        BS[r, :N] = bg * BCS[r, :N]
        BS[r, N:] = cg * BCS[r, N:]
        return carry

    shared(0, 0)
    HSB[0] = BS[0:8, :]
    halo_bs = send(HSB.at[0], HSB.at[1], s_sl.at[0], r_sl.at[0], at_seq(s - 1))

    @pl.when(s > 0)
    def _():
        halo_bs.start()

    lax.fori_loop(1, nb, shared, 0)

    def tap_sums(slope, F, start, carry):
        n = slope.shape[0]
        v = F[pl.ds(pl.multiple_of(start, 8), n + 8), :]
        out = []
        for k in range(TAPS):
            moved = v[8:, :] if k == 0 else pltpu.roll(v, k, 0)[8:, :]
            out.append(carry[k] + (slope * moved).reshape(n // 8, 8, W).sum(axis=0))
        return tuple(out)

    def stack_taps(sums):
        rt8 = lax.broadcasted_iota(jnp.int32, (8, W), 0)
        out = jnp.zeros((8, W), F32)
        for k in range(TAPS):
            out = jnp.where(rt8 == k, jnp.sum(sums[k], axis=0, keepdims=True), out)
        return out

    zero4 = tuple(jnp.zeros((8, W), F32) for _ in range(TAPS))
    sums = lax.fori_loop(
        0, T // CH, lambda i, cr: tap_sums(BS[blk(i, CH), :], BCF, i * CH, cr), zero4
    )
    CBS[s] = stack_taps(sums)

    def seq_copy(buf, d, ss, rs):
        p, _ = other(d)
        return send(buf.at[s], buf.at[s], ss.at[d], rs.at[s], at_seq(p))

    def seq_wait(buf, ss, rs):
        for d in range(1, nseq):
            p, _ = other(d)
            send(buf.at[p], buf.at[p], ss.at[d], rs.at[p], at_seq(p)).wait_recv()

    for d in range(1, nseq):
        seq_copy(CBS, d, s_cb, r_cb).start()

    groups = nz * nyl * nc
    per_block = groups // nb
    zy_block = per_block // nc

    def bc_adjoint(j, carry):
        u = BS[pl.ds(pl.multiple_of(j * own, 8), own + 8), :]
        out = cvb[0:1, :] * u[:own, :]
        for k in range(1, TAPS):
            out = out + cvb[k : k + 1, :] * pltpu.roll(u, own + 8 - k, 0)[:own, :]
        PR[j // nc, lax.rem(j, nc)] = out.astype(BF16)
        return carry

    def a_copy(q):
        part = pl.ds(q * zy_block, zy_block)
        return send(PR.at[part, 1 - c], RA.at[part], s_a.at[q], r_a.at[q], core_dev)

    for q in range(nb):
        if q == nb - 1:

            @pl.when(s < nseq - 1)
            def _():
                halo_bs.wait_recv()
                BS[T : T + 8, :] = HSB[1]

            @pl.when(s == nseq - 1)
            def _():
                BS[T : T + 8, :] = jnp.zeros((8, W), F32)

        lax.fori_loop(q * per_block, (q + 1) * per_block, bc_adjoint, 0)
        a_copy(q).start()

    CW = 128
    lane1 = lax.broadcasted_iota(jnp.int32, (1, W), 1) // HEAD_DIM
    skip = by_head([d_s[h] for h in range(heads)], lane1)
    pick = (
        lax.broadcasted_iota(jnp.int32, (16, W), 0)
        == lax.broadcasted_iota(jnp.int32, (16, W), 1) // HEAD_DIM
    ).astype(F32).astype(BF16)

    def channels(i, carry):
        r = blk(i, CW)
        k = i // (BLOCK // CW)
        wg = WGIN[r, :] + LEA[r, :] * mm(BCP[r, :N], GB[k])
        xp = XP[r, :].astype(F32)
        slope = (DTE[r, :] * wg + skip * DY[r, :].astype(F32)) * XS[r, :]
        XSL[r, :] = slope
        prod = xp * wg
        hi = prod.astype(BF16)
        lo = (prod - hi.astype(F32)).astype(BF16)
        steps = mm(pick, hi, NT) + mm(pick, lo, NT)
        sg_o[:, pl.ds(pl.multiple_of(i * CW, CW), CW)] = steps[0:heads, :]
        return tap_sums(slope, XF, i * CW, carry)

    sums = channels(0, zero4)
    HSX[0] = XSL[0:8, :]
    halo_xs = send(HSX.at[0], HSX.at[1], s_sl.at[1], r_sl.at[1], at_seq(s - 1))

    @pl.when(s > 0)
    def _():
        halo_xs.start()

    def b_step(q):
        zs = nz // nb
        for zi in range(zs):
            zz = q * zs + zi
            A1S[zz] = (
                PR[zz * nyl + 1 - yl, c].astype(F32) + RA[zz * nyl + 1 - yl].astype(F32)
            ).astype(BF16)
            A1K[zz] = PR[zz * nyl + yl, c].astype(F32) + RA[zz * nyl + yl].astype(F32)

    def b_copy(q):
        part = pl.ds(q * (nz // nb), nz // nb)
        return send(A1S.at[part], RB.at[part], s_b.at[q], r_b.at[q], y_dev)

    per_q = (T // CW) // nb
    for q in range(nb):
        sums = lax.fori_loop(max(1, q * per_q), (q + 1) * per_q, channels, sums)
        a_copy(q).wait_recv()
        b_step(q)
        b_copy(q).start()
    CXS[s] = stack_taps(sums)
    for d in range(1, nseq):
        seq_copy(CXS, d, s_cx, r_cx).start()

    def total8(buf, n):
        out = buf[0]
        for p in range(1, n):
            out = out + buf[p]
        return out

    seq_wait(CBS, s_cb, r_cb)
    CBL[0] = total8(CBS, nseq)
    cc_copy = send(CBL.at[0], CBL.at[1], s_cc.at[0], r_cc.at[0], core_dev)
    cc_copy.start()

    def outputs(i, carry):
        r = blk(i, CH)
        k = i // (BLOCK // CH)
        y = YIN[r, :] + ENT[r, :] * mm(BCP[r, N:], SB[k]) + skip * XP[r, :].astype(F32)
        gg_o[r, :] = (GZ[r, :] * y).astype(BF16)
        return carry

    lax.fori_loop(0, T // CH // 2, outputs, 0)

    for q in range(nb):
        b_copy(q).wait_recv()
    for zz in range(nz):
        val = A1K[zz] + RB[zz].astype(F32)
        A2[zz] = val
        ZS[zz] = val.astype(BF16)

    def z_copy(d):
        t = other_z(d)
        return send(ZS.at[t], RZ.at[z], s_z.at[d], r_z.at[z], {"head_0": t})

    for d in range(1, nz):
        z_copy(d).start()

    cc_copy.wait_recv()
    CBT[0] = CBL[0] + CBL[1]
    cy_copy = send(CBT.at[0], CBT.at[1], s_cc.at[1], r_cc.at[1], y_dev)
    cy_copy.start()

    lax.fori_loop(T // CH // 2, T // CH, outputs, 0)

    def x_adjoint(i, carry):
        r = blk(i, CH)
        u = XSL[pl.ds(pl.multiple_of(i * CH, 8), CH + 8), :]
        out = cvx[0:1, :] * u[:CH, :]
        for k in range(1, TAPS):
            out = out + cvx[k : k + 1, :] * pltpu.roll(u, CH + 8 - k, 0)[:CH, :]
        xg_o[r, :] = out.astype(BF16)
        return carry

    @pl.when(s < nseq - 1)
    def _():
        halo_xs.wait_recv()
        XSL[T : T + 8, :] = HSX[1]

    @pl.when(s == nseq - 1)
    def _():
        XSL[T : T + 8, :] = jnp.zeros((8, W), F32)

    cy_copy.wait_recv()
    CBZ[z] = CBT[0] + CBT[1]

    def cz_copy(d):
        return send(CBZ.at[z], CBZ.at[z], s_cz.at[d], r_cz.at[z], {"head_0": other_z(d)})

    for d in range(1, nz):
        cz_copy(d).start()

    lax.fori_loop(0, T // CH, x_adjoint, 0)

    seq_wait(CXS, s_cx, r_cx)
    cx_o[...] = total8(CXS, nseq)[0:TAPS, :]
    out = A2[z]
    for d in range(1, nz):
        t = other_z(d)
        send(ZS.at[t], RZ.at[t], s_z.at[d], r_z.at[t], {"head_0": t}).wait_recv()
        out = out + RZ[t].astype(F32)
    bg_o[...] = out
    for d in range(1, nz):
        t = other_z(d)
        send(CBZ.at[t], CBZ.at[t], s_cz.at[d], r_cz.at[t], {"head_0": t}).wait_recv()
    cb_o[...] = total8(CBZ, nz)[0:TAPS, :]

    @pl.when(s < nseq - 1)
    def _():
        halo_x.wait_send()
        halo_b.wait_send()

    @pl.when(s > 0)
    def _():
        halo_bs.wait_send()
        halo_xs.wait_send()

    for d in range(1, nseq):
        state_copy(d).wait_send()
        seq_copy(CBS, d, s_cb, r_cb).wait_send()
        seq_copy(CXS, d, s_cx, r_cx).wait_send()
    for q in range(nb):
        a_copy(q).wait_send()
        b_copy(q).wait_send()
    for d in range(1, nz):
        z_copy(d).wait_send()
        cz_copy(d).wait_send()
    cc_copy.wait_send()
    cy_copy.wait_send()


def local(dims, xraw, zgate, bcraw, dt, a_rate, d_skip, conv_x, conv_bc, dout):
    nx, nyh, nz, nyl, nc = dims
    nseq = nx * nyh
    T, W = xraw.shape
    nb = T // BLOCK
    heads = W // HEAD_DIM
    N = W // 2
    own = T // (nz * nyl * nc)
    vm = lambda *shape: pltpu.VMEM(shape[:-1], shape[-1])
    full, half = vm(T, W, F32), vm(T, W, BF16)
    ext = vm(T + 8, W, F32)
    dma = lambda n: pltpu.SemaphoreType.DMA((n,))
    scratch = (
        [ext, ext] + [full] * 8 + [ext, ext]
        + [half] * 5 + [half, vm(T, BLOCK, BF16)]
        + [vm(nb * heads, BLOCK, F32), vm(nb * heads, BLOCK, F32), vm(3 * nb * heads, BLOCK, BF16)]
        + [vm(nb, 8, W, F32)]
        + [vm(nb, N, W, F32)] * 4
        + [vm(nb, N, W, BF16)] * 2
        + [vm(2, N + 16, W, BF16), vm(nseq, N + 16, W, BF16)]
        + [vm(BLOCK, heads * BLOCK, BF16), vm(heads * BLOCK, W, BF16), vm(heads * BLOCK, W, BF16)]
        + [vm(16, W, BF16)] * 2 + [vm(2, 8, W, F32)] * 2
        + [vm(nz * nyl, nc, own, W, BF16), vm(nz * nyl, own, W, BF16)]
        + [vm(nz, own, W, BF16), vm(nz, own, W, F32), vm(nz, own, W, BF16), vm(nz, own, W, F32)]
        + [vm(nz, own, W, BF16), vm(nz, own, W, BF16)]
        + [vm(nseq, 8, W, F32)] * 2 + [vm(2, 8, W, F32)] * 2 + [vm(nz, 8, W, F32)]
        + [dma(2)] * 2 + [dma(nseq)] * 2 + [dma(2)] * 2 + [dma(nb)] * 4 + [dma(nz)] * 2
        + [dma(nseq)] * 4 + [dma(2)] * 2 + [dma(nz)] * 2
    )
    vspec = pl.BlockSpec(memory_space=pltpu.VMEM)
    sspec = pl.BlockSpec(memory_space=pltpu.SMEM)
    return pl.pallas_call(
        functools.partial(kernel, dims, T, W),
        name="ssd_backward",
        out_shape=(
            jax.ShapeDtypeStruct((T, W), BF16),
            jax.ShapeDtypeStruct((T, W), BF16),
            jax.ShapeDtypeStruct((heads, T), F32),
            jax.ShapeDtypeStruct((own, W), F32),
            jax.ShapeDtypeStruct((TAPS, W), F32),
            jax.ShapeDtypeStruct((TAPS, W), F32),
        ),
        in_specs=[vspec, vspec, vspec, vspec, sspec, sspec, vspec, vspec, vspec],
        out_specs=tuple([vspec] * 6),
        scratch_shapes=scratch,
        compiler_params=pltpu.CompilerParams(
            collective_id=0, has_side_effects=True, vmem_limit_bytes=56 * 1024 * 1024
        ),
    )(xraw, zgate, bcraw, dt, a_rate, d_skip, conv_x, conv_bc, dout)


def over_mesh(torus):
    placed = (
        P(SEQ, HEAD), P(SEQ, HEAD), P(SEQ, None), P(HEAD, SEQ), P(HEAD), P(HEAD),
        P(None, HEAD), P(), P(SEQ, HEAD),
    )
    return jax.shard_map(
        functools.partial(local, tuple(torus.devices.shape)),
        mesh=torus,
        in_specs=placed,
        out_specs=(P(SEQ, HEAD), P(SEQ, HEAD), P(HEAD, SEQ), P(SEQ_HEAD, None), P(None, HEAD), P()),
        check_vma=False,
    )


def solution(mesh):
    return over_mesh(Mesh(mesh.devices.reshape(4, 2, 8, 2, 2), SEQ_HEAD))
```

```python
import functools

import jax
import jax.numpy as jnp
from jax import lax
from jax.experimental import pallas as pl
from jax.experimental.pallas import tpu as pltpu
from jax.sharding import Mesh
from jax.sharding import PartitionSpec as P

HEAD_DIM = 64
BLOCK = 256
TAPS = 4
SEQ = ("seq_0", "seq_1")
HEAD = ("head_0", "head_1", "head_2")
SEQ_HEAD = SEQ + HEAD
F32, BF16 = jnp.float32, jnp.bfloat16


def mm(a, b, dims=((1,), (0,))):
    return lax.dot_general(a, b, (dims, ((), ())), preferred_element_type=F32)


NT = ((1,), (1,))
TN = ((0,), (0,))


def parts3(v):
    p1 = v.astype(BF16)
    r1 = v - p1.astype(F32)
    p2 = r1.astype(BF16)
    r2 = r1 - p2.astype(F32)
    return p1, p2, r2.astype(BF16)


def sigmoid(v):
    return 0.5 * jnp.tanh(0.5 * v) + 0.5


def silu_slope(v):
    q = sigmoid(v)
    return q * (1.0 + v * (1.0 - q))


def by_head(scalars, lanes):
    out = jnp.full(lanes.shape, scalars[3], F32)
    for h in (2, 1, 0):
        out = jnp.where(lanes == h, scalars[h], out)
    return out


def kernel(
    dims, T, W,
    xraw_h, zg_h, bcr_h, dt_h, a_s, d_s, cvx_h, cvb_h, dout_h,
    xg_o, gg_o, sg_o, bg_o, cx_o, cb_o,
    xraw, zg, bcr, dt, cvx, cvb, dout,
    XF, BCF, XS, BCS, GZ, DTE, ENT, LEA, YIN, WGIN, XSL, BS,
    XP, WX, WL, DY, DYE, BCP, MX,
    GC, DC, WP, TOT, EK, BK, LS, NS, SB, GB, EB, SLOT, CR, CSLOT,
    KH, WXM, DYM, HXR, HBR, HSX, HSB,
    PR, RA, ZS, RZ, CXS, CBS, CBL, CBZ,
    s_in, s_h, r_h, s_st, r_st, s_cr, r_cr, s_sl, r_sl, s_a, r_a, s_z, r_z,
    s_cx, r_cx, s_cb, r_cb, s_cc, r_cc, s_cz, r_cz,
):
    nx, nyh, nz, nyl, nc = dims
    nseq = nx * nyh
    nzy = nz * nyl
    nb = T // BLOCK
    heads = W // HEAD_DIM
    own = T // (nzy * nc)
    sx, sy = lax.axis_index("seq_0"), lax.axis_index("seq_1")
    s = sx * nyh + sy
    z, yl, c = (lax.axis_index(n) for n in HEAD)
    m = z * nyl + yl

    def at_seq(p):
        return {"seq_0": p // nyh, "seq_1": lax.rem(p, nyh)}

    def at_zy(p):
        return {"head_0": p // nyl, "head_1": lax.rem(p, nyl)}

    def other(d):
        wrapped = (s + d) // nseq
        return s + d - nseq * wrapped, wrapped

    def other_zy(d):
        return lax.rem(m + d, nzy)

    far_first = sorted(range(1, nzy), key=lambda d: -min(d, nzy - d))

    def send(src, dst, ss, rs, dev):
        return pltpu.make_async_remote_copy(
            src_ref=src, dst_ref=dst, send_sem=ss, recv_sem=rs,
            device_id=dev, device_id_type=pl.DeviceIdType.MESH,
        )

    core_dev = {"head_2": 1 - c}

    barrier = pltpu.get_barrier_semaphore()

    def greet(dev):
        pl.semaphore_signal(barrier, inc=1, device_id=dev, device_id_type=pl.DeviceIdType.MESH)

    for d in range(1, nseq):
        greet(at_seq(other(d)[0]))
    for d in far_first:
        greet(at_zy(other_zy(d)))
    greet(core_dev)

    loads = [
        pltpu.make_async_copy(a, b, s_in.at[i])
        for i, (a, b) in enumerate(
            [(dt_h, dt), (zg_h, zg), (dout_h, dout), (bcr_h, bcr), (xraw_h, xraw),
             (cvx_h, cvx), (cvb_h, cvb)]
        )
    ]
    for load in loads:
        load.start()

    rows16 = lax.broadcasted_iota(jnp.int32, (heads, BLOCK), 0)
    a_col = by_head([a_s[h] for h in range(heads)], rows16)
    n16 = nb * heads
    ri = lax.broadcasted_iota(jnp.int32, (BLOCK, BLOCK), 0)
    ci = lax.broadcasted_iota(jnp.int32, (BLOCK, BLOCK), 1)
    tri = (ri <= ci).astype(F32).astype(BF16)
    rr = lax.rem(lax.broadcasted_iota(jnp.int32, (3 * n16, W), 0), n16)
    ll = lax.broadcasted_iota(jnp.int32, (3 * n16, W), 1) // HEAD_DIM
    loads[0].wait()
    for k in range(nb):
        piece = dt[:, k * BLOCK : (k + 1) * BLOCK]
        DC[k * heads : (k + 1) * heads, :] = piece
        GC[k * heads : (k + 1) * heads, :] = piece * a_col
    w3 = mm(jnp.concatenate(parts3(GC[...]), axis=0), tri)
    within = w3[:n16] + w3[n16 : 2 * n16] + w3[2 * n16 :]
    GC[...] = within
    wp = jnp.concatenate(parts3(within), axis=0)
    dp = jnp.concatenate(parts3(DC[...]), axis=0)
    WP[...] = wp

    def blk(k, n=BLOCK):
        return pl.ds(pl.multiple_of(k * n, n), n)

    def expand(k, carry):
        hot = ((rr // heads == k) & (lax.rem(rr, heads) == ll)).astype(F32).astype(BF16)
        wexp = mm(wp, hot, TN)
        total = wexp[BLOCK - 1 : BLOCK, :]
        TOT[k] = jnp.broadcast_to(total, (8, W))
        ENT[blk(k), :] = jnp.exp(-wexp)
        LEA[blk(k), :] = jnp.exp(jnp.minimum(wexp - total, 0.0))
        DTE[blk(k), :] = mm(dp, hot, TN)
        return carry

    lax.fori_loop(0, nb, expand, 0)

    CH = 64
    N = W // 2
    per = BLOCK // CH
    for load in loads[1:]:
        load.wait()
    XF[0:8, :] = jnp.zeros((8, W), F32)
    BCF[0:8, :] = jnp.zeros((8, W), F32)

    def gates(i, carry):
        r = blk(i, CH)
        zv = zg[r, :].astype(F32)
        dy = (dout[r, :].astype(F32) * (zv * sigmoid(zv))).astype(BF16)
        DY[r, :] = dy
        DYE[r, :] = (dy.astype(F32) * ENT[r, :]).astype(BF16)
        shifted = pl.ds(pl.multiple_of(8 + i * CH, 8), CH)
        XF[shifted, :] = xraw[r, :].astype(F32)
        BCF[shifted, :] = bcr[r, :].astype(F32)
        return carry

    lax.fori_loop(0, T // CH, gates, 0)

    def conv_chunk(i, carry):
        r = blk(i, CH)
        ext = pl.ds(pl.multiple_of(i * CH, 8), CH + 8)

        def pre(F, taps):
            v = F[ext, :]
            out = taps[0:1, :] * v[8:, :]
            for k in range(1, TAPS):
                out = out + taps[k : k + 1, :] * pltpu.roll(v, k, 0)[8:, :]
            return out

        v = pre(BCF, cvb)
        BCP[r, :] = (v * sigmoid(v)).astype(BF16)
        BCS[r, :] = v
        v = pre(XF, cvx)
        post = (v * sigmoid(v)).astype(BF16)
        XP[r, :] = post
        XS[r, :] = v
        wx = (post.astype(F32) * DTE[r, :]).astype(BF16)
        WX[r, :] = wx
        WL[r, :] = (wx.astype(F32) * LEA[r, :]).astype(BF16)
        return carry

    def block_ends(k, carry):
        EK[k] = mm(BCP[blk(k), :N], WL[blk(k), :], TN)
        BK[k] = mm(BCP[blk(k), N:], DYE[blk(k), :], TN)
        return carry

    lax.fori_loop(0, T // CH, conv_chunk, 0)
    rt = lax.broadcasted_iota(jnp.int32, (16, W), 0)
    edge = rt < TAPS - 1
    BCP[0:16, :] = jnp.where(edge, jnp.zeros((16, W), BF16), BCP[0:16, :])
    lax.fori_loop(0, nb, block_ends, 0)

    state = jnp.zeros((N, W), F32)
    for k in range(nb):
        LS[k] = state
        state = jnp.exp(-TOT[k][0:1, :]) * state + EK[k]
    EB[0] = state.astype(BF16)
    grad = jnp.zeros((N, W), F32)
    for k in reversed(range(nb)):
        NS[k] = grad
        grad = jnp.exp(-TOT[k][0:1, :]) * grad + BK[k]
    EB[1] = grad.astype(BF16)

    pl.semaphore_wait(barrier, nseq - 1 + nzy - 1 + 1)

    halo_x = send(xraw.at[T - 16 :], HXR, s_h.at[0], r_h.at[0], at_seq(s + 1))
    halo_b = send(bcr.at[T - 16 :], HBR, s_h.at[1], r_h.at[1], at_seq(s + 1))

    @pl.when(s < nseq - 1)
    def _():
        halo_x.start()
        halo_b.start()

    def state_copy(d):
        p, wrapped = other(d)
        return send(EB.at[wrapped], SLOT.at[s], s_st.at[d], r_st.at[s], at_seq(p))

    def edge_copy(d):
        p, wrapped = other(d)
        return send(CR.at[wrapped], CSLOT.at[s], s_cr.at[d], r_cr.at[s], at_seq(p))

    for d in range(1, nseq):
        state_copy(d).start()

    lane_h = lax.broadcasted_iota(jnp.int32, (BLOCK, W), 1) // HEAD_DIM
    r512 = lax.rem(lax.broadcasted_iota(jnp.int32, (3 * n16, heads * 128), 0), n16)
    l512 = lax.broadcasted_iota(jnp.int32, (3 * n16, heads * 128), 1) // 128
    for h in range(heads):
        KH[0:128, h * BLOCK + 128 : (h + 1) * BLOCK] = jnp.zeros((128, 128), BF16)
    TQ = 64

    def inside(k, carry):
        bm, cm = BCP[blk(k), :N], BCP[blk(k), N:]
        wx, dy = WX[blk(k), :], DY[blk(k), :]
        for h in range(heads):
            WXM[h * BLOCK : (h + 1) * BLOCK, :] = jnp.where(lane_h == h, wx, jnp.zeros_like(wx))
            DYM[h * BLOCK : (h + 1) * BLOCK, :] = jnp.where(lane_h == h, dy, jnp.zeros_like(dy))
        hot = ((r512 // heads == k) & (lax.rem(r512, heads) == l512)).astype(F32).astype(BF16)
        col = mm(WP[...], hot, TN)
        for t0 in range(0, BLOCK, TQ):
            ext = 128 if t0 < 128 else BLOCK
            sc = mm(cm[t0 : t0 + TQ, :], bm[0:ext, :], NT)
            tt = t0 + lax.broadcasted_iota(jnp.int32, (TQ, ext), 0)
            ss = lax.broadcasted_iota(jnp.int32, (TQ, ext), 1)
            keep = tt >= ss
            total = None
            for h in range(heads):
                wrow = GC[pl.ds(k * heads + h, 1), :][:, 0:ext]
                wcol = col[t0 : t0 + TQ, h * 128 : (h + 1) * 128]
                if ext > 128:
                    wcol = jnp.concatenate([wcol, wcol], axis=1)
                decay = jnp.where(keep, jnp.exp(jnp.minimum(wrow - wcol, 0.0)), 0.0)
                KH[t0 : t0 + TQ, h * BLOCK : h * BLOCK + ext] = (sc * decay).astype(BF16)
                mixing = mm(DYM[h * BLOCK + t0 : h * BLOCK + t0 + TQ, :], wx[0:ext, :], NT)
                part = mixing * decay
                total = part if total is None else total + part
            rows = pl.ds(pl.multiple_of(k * BLOCK + t0, TQ), TQ)
            MX[rows, 0:ext] = total.astype(BF16)
            if ext < BLOCK:
                MX[rows, ext:] = jnp.zeros((TQ, BLOCK - ext), BF16)
        YIN[blk(k), :] = mm(KH[...], WXM[...])
        acc = None
        for h in range(heads):
            part = mm(KH[:, h * BLOCK : (h + 1) * BLOCK], DYM[h * BLOCK : (h + 1) * BLOCK, :], TN)
            acc = part if acc is None else acc + part
        WGIN[blk(k), :] = acc
        return carry

    lax.fori_loop(nb - 2, nb, inside, 0)

    @pl.when(s > 0)
    def _():
        halo_x.wait_recv()
        halo_b.wait_recv()
        XF[0:8, :] = HXR[8:16, :].astype(F32)
        BCF[0:8, :] = HBR[8:16, :].astype(F32)

    conv_chunk(0, 0)
    dtot = TOT[0][0:1, :]
    for k in range(1, nb):
        dtot = dtot + TOT[k][0:1, :]
    tail0 = TOT[0][0:1, :]
    q1, q2, q3 = (p.astype(F32) for p in parts3(dtot))

    def edge_rows(v):
        v = jnp.where(edge, v, 0.0)
        v = jnp.where(rt == 8, q1, jnp.where(rt == 9, q2, jnp.where(rt == 10, q3, v)))
        return v.astype(BF16)

    CR[0, :, 0:W] = edge_rows(
        WX[0:16, :].astype(F32) * LEA[0:16, :] * jnp.exp(jnp.minimum(tail0 - dtot, 0.0))
    )
    CR[1, :, 0:W] = edge_rows(DYE[0:16, :].astype(F32))
    first = jnp.where(edge, BCP[0:16, :], jnp.zeros((16, W), BF16))
    CR[0, :, W:] = first[:, :N]
    CR[1, :, W:] = first[:, N:]
    for d in range(1, nseq):
        edge_copy(d).start()
    start0 = mm(first[:, :N], WL[0:16, :], TN)

    lax.fori_loop(0, nb - 2, inside, 0)

    def slopes(i, carry):
        r = blk(i, CH)
        BCS[r, :] = silu_slope(BCS[r, :])
        XS[r, :] = silu_slope(XS[r, :])
        GZ[r, :] = dout[r, :].astype(F32) * silu_slope(zg[r, :].astype(F32))
        return carry

    lax.fori_loop(0, T // CH, slopes, 0)

    def mixed(k, carry):
        r = blk(k)
        mx = MX[r, :]
        BS[r, :N] = mm(mx, BCP[r, N:], TN)
        BS[r, N:] = mm(mx, BCP[r, :N])
        return carry

    lax.fori_loop(0, nb, mixed, 0)

    for d in range(1, nseq):
        p, _ = other(d)
        send(EB.at[0], SLOT.at[p], s_st.at[d], r_st.at[p], at_seq(p)).wait_recv()
        send(CR.at[0], CSLOT.at[p], s_cr.at[d], r_cr.at[p], at_seq(p)).wait_recv()

    def fold(p, value):
        rows = CSLOT[p, :, 0:W]
        t3 = rows[8:16, :].astype(F32)
        dec = jnp.exp(-(t3[0:1, :] + t3[1:2, :] + t3[2:3, :]))
        late = mm(CSLOT[p, :, W:], rows, TN)
        return dec * value + (SLOT[p].astype(F32) + late)

    s_first = lax.fori_loop(0, s, fold, jnp.zeros((N, W), F32))
    g_last = lax.fori_loop(0, nseq - 1 - s, lambda i, v: fold(nseq - 1 - i, v), jnp.zeros((N, W), F32))
    SB[0] = s_first.astype(BF16)
    s_next = jnp.exp(-TOT[0][0:1, :]) * s_first + start0
    before = jnp.zeros((1, W), F32)
    for k in range(1, nb):
        SB[k] = (LS[k] + jnp.exp(-before) * s_next).astype(BF16)
        before = before + TOT[k][0:1, :]
    after = jnp.zeros((1, W), F32)
    for k in reversed(range(nb)):
        GB[k] = (NS[k] + jnp.exp(-after) * g_last).astype(BF16)
        after = after + TOT[k][0:1, :]

    def shared(k, carry):
        r = blk(k)
        BS[r, :N] = (BS[r, :N] + mm(WL[r, :], GB[k], NT)) * BCS[r, :N]
        BS[r, N:] = (BS[r, N:] + mm(DYE[r, :], SB[k], NT)) * BCS[r, N:]
        return carry

    shared(0, 0)
    HSB[0] = BS[0:8, :]
    halo_bs = send(HSB.at[0], HSB.at[1], s_sl.at[0], r_sl.at[0], at_seq(s - 1))

    @pl.when(s > 0)
    def _():
        halo_bs.start()

    lax.fori_loop(1, nb, shared, 0)

    def bc_adjoint(j, carry):
        u = BS[pl.ds(pl.multiple_of(j * own, 8), own + 8), :]
        out = cvb[0:1, :] * u[:own, :]
        for k in range(1, TAPS):
            out = out + cvb[k : k + 1, :] * pltpu.roll(u, own + 8 - k, 0)[:own, :]
        PR[j // nc, lax.rem(j, nc)] = out.astype(BF16)
        return carry

    pieces = [(0, nzy // 2), (nzy // 2, nzy - 1), (nzy - 1, nzy)]

    def a_copy(q):
        lo, hi = pieces[q]
        part = pl.ds(lo, hi - lo)
        return send(PR.at[part, 1 - c], RA.at[part], s_a.at[q], r_a.at[q], core_dev)

    def adjoint_piece(q):
        lax.fori_loop(pieces[q][0] * nc, pieces[q][1] * nc, bc_adjoint, 0)
        a_copy(q).start()

    def pair_sum(i, carry):
        ZS[i] = (PR[i, c].astype(F32) + RA[i].astype(F32)).astype(BF16)
        return carry

    def z_copy(d):
        t = other_zy(d)
        return send(ZS.at[t], RZ.at[m], s_z.at[d], r_z.at[m], at_zy(t))

    adjoint_piece(0)
    adjoint_piece(1)

    def tap_sums(slope, F, start, carry):
        n = slope.shape[0]
        v = F[pl.ds(pl.multiple_of(start, 8), n + 8), :]
        out = []
        for k in range(TAPS):
            moved = v[8:, :] if k == 0 else pltpu.roll(v, k, 0)[8:, :]
            out.append(carry[k] + (slope * moved).reshape(n // 8, 8, W).sum(axis=0))
        return tuple(out)

    def stack_taps(sums):
        rt8 = lax.broadcasted_iota(jnp.int32, (8, W), 0)
        out = jnp.zeros((8, W), F32)
        for k in range(TAPS):
            out = jnp.where(rt8 == k, jnp.sum(sums[k], axis=0, keepdims=True), out)
        return out

    zero4 = tuple(jnp.zeros((8, W), F32) for _ in range(TAPS))
    sums = lax.fori_loop(
        0, T // CH, lambda i, cr: tap_sums(BS[blk(i, CH), :], BCF, i * CH, cr), zero4
    )
    CBS[s] = stack_taps(sums)

    def seq_copy(buf, d, ss, rs):
        p, _ = other(d)
        return send(buf.at[s], buf.at[s], ss.at[d], rs.at[s], at_seq(p))

    def seq_wait(buf, ss, rs):
        for d in range(1, nseq):
            p, _ = other(d)
            send(buf.at[p], buf.at[p], ss.at[d], rs.at[p], at_seq(p)).wait_recv()

    for d in range(1, nseq):
        seq_copy(CBS, d, s_cb, r_cb).start()

    CW = 128
    lane1 = lax.broadcasted_iota(jnp.int32, (1, W), 1) // HEAD_DIM
    skip = by_head([d_s[h] for h in range(heads)], lane1)
    pick = (
        lax.broadcasted_iota(jnp.int32, (16, W), 0)
        == lax.broadcasted_iota(jnp.int32, (16, W), 1) // HEAD_DIM
    ).astype(F32).astype(BF16)

    def channels(i, carry):
        r = blk(i, CW)
        k = i // (BLOCK // CW)
        wg = WGIN[r, :] + LEA[r, :] * mm(BCP[r, :N], GB[k])
        xp = XP[r, :].astype(F32)
        slope = (DTE[r, :] * wg + skip * DY[r, :].astype(F32)) * XS[r, :]
        XSL[r, :] = slope
        prod = xp * wg
        hi = prod.astype(BF16)
        lo = (prod - hi.astype(F32)).astype(BF16)
        steps = mm(pick, hi, NT) + mm(pick, lo, NT)
        sg_o[:, pl.ds(pl.multiple_of(i * CW, CW), CW)] = steps[0:heads, :]
        return tap_sums(slope, XF, i * CW, carry)

    sums = channels(0, zero4)
    HSX[0] = XSL[0:8, :]
    halo_xs = send(HSX.at[0], HSX.at[1], s_sl.at[1], r_sl.at[1], at_seq(s - 1))

    @pl.when(s > 0)
    def _():
        halo_xs.start()

    for q in range(2):
        a_copy(q).wait_recv()
        lax.fori_loop(pieces[q][0], pieces[q][1], pair_sum, 0)
    for d in far_first:

        @pl.when(other_zy(d) < nzy - 1)
        def _():
            z_copy(d).start()

    sums = lax.fori_loop(1, 3, channels, sums)

    @pl.when(s < nseq - 1)
    def _():
        halo_bs.wait_recv()
        BS[T : T + 8, :] = HSB[1]

    @pl.when(s == nseq - 1)
    def _():
        BS[T : T + 8, :] = jnp.zeros((8, W), F32)

    adjoint_piece(2)
    sums = lax.fori_loop(3, 6, channels, sums)
    a_copy(2).wait_recv()
    pair_sum(nzy - 1, 0)

    @pl.when(m < nzy - 1)
    def _():
        z_copy(nzy - 1 - m).start()

    sums = lax.fori_loop(6, T // CW, channels, sums)
    CXS[s] = stack_taps(sums)
    for d in range(1, nseq):
        seq_copy(CXS, d, s_cx, r_cx).start()

    def total8(buf, n):
        out = buf[0]
        for p in range(1, n):
            out = out + buf[p]
        return out

    seq_wait(CBS, s_cb, r_cb)
    CBL[0] = total8(CBS, nseq)
    cc_copy = send(CBL.at[0], CBL.at[1], s_cc.at[0], r_cc.at[0], core_dev)
    cc_copy.start()

    def outputs(i, carry):
        r = blk(i, CH)
        k = i // (BLOCK // CH)
        y = YIN[r, :] + ENT[r, :] * mm(BCP[r, N:], SB[k]) + skip * XP[r, :].astype(F32)
        gg_o[r, :] = (GZ[r, :] * y).astype(BF16)
        return carry

    lax.fori_loop(0, T // CH // 2, outputs, 0)

    cc_copy.wait_recv()
    CBZ[m] = CBL[0] + CBL[1]

    def cz_copy(d):
        return send(CBZ.at[m], CBZ.at[m], s_cz.at[d], r_cz.at[m], at_zy(other_zy(d)))

    for d in far_first:
        cz_copy(d).start()

    lax.fori_loop(T // CH // 2, T // CH, outputs, 0)

    def x_adjoint(i, carry):
        r = blk(i, CH)
        u = XSL[pl.ds(pl.multiple_of(i * CH, 8), CH + 8), :]
        out = cvx[0:1, :] * u[:CH, :]
        for k in range(1, TAPS):
            out = out + cvx[k : k + 1, :] * pltpu.roll(u, CH + 8 - k, 0)[:CH, :]
        xg_o[r, :] = out.astype(BF16)
        return carry

    @pl.when(s < nseq - 1)
    def _():
        halo_xs.wait_recv()
        XSL[T : T + 8, :] = HSX[1]

    @pl.when(s == nseq - 1)
    def _():
        XSL[T : T + 8, :] = jnp.zeros((8, W), F32)

    lax.fori_loop(0, T // CH, x_adjoint, 0)

    seq_wait(CXS, s_cx, r_cx)
    cx_o[...] = total8(CXS, nseq)[0:TAPS, :]
    out = PR[m, c].astype(F32) + RA[m].astype(F32)
    for d in range(1, nzy):
        t = other_zy(d)
        send(ZS.at[t], RZ.at[t], s_z.at[d], r_z.at[t], at_zy(t)).wait_recv()
        out = out + RZ[t].astype(F32)
    bg_o[...] = out
    for d in range(1, nzy):
        t = other_zy(d)
        send(CBZ.at[t], CBZ.at[t], s_cz.at[d], r_cz.at[t], at_zy(t)).wait_recv()
    cb_o[...] = total8(CBZ, nzy)[0:TAPS, :]

    @pl.when(s < nseq - 1)
    def _():
        halo_x.wait_send()
        halo_b.wait_send()

    @pl.when(s > 0)
    def _():
        halo_bs.wait_send()
        halo_xs.wait_send()

    for d in range(1, nseq):
        state_copy(d).wait_send()
        edge_copy(d).wait_send()
        seq_copy(CBS, d, s_cb, r_cb).wait_send()
        seq_copy(CXS, d, s_cx, r_cx).wait_send()
    for q in range(3):
        a_copy(q).wait_send()
    for d in range(1, nzy):
        z_copy(d).wait_send()
        cz_copy(d).wait_send()
    cc_copy.wait_send()


def emit(*refs):
    held, outs, sem = refs[:6], refs[6:12], refs[12]
    copies = [pltpu.make_async_copy(a, b, sem.at[i]) for i, (a, b) in enumerate(zip(held, outs))]
    for copy in copies:
        copy.start()
    for copy in copies:
        copy.wait()


def local(dims, xraw, zgate, bcraw, dt, a_rate, d_skip, conv_x, conv_bc, dout):
    nx, nyh, nz, nyl, nc = dims
    nseq = nx * nyh
    nzy = nz * nyl
    T, W = xraw.shape
    nb = T // BLOCK
    heads = W // HEAD_DIM
    N = W // 2
    own = T // (nzy * nc)
    vm = lambda *shape: pltpu.VMEM(shape[:-1], shape[-1])
    full, half = vm(T, W, F32), vm(T, W, BF16)
    ext = vm(T + 8, W, F32)
    taps = vm(TAPS, W, F32)
    dma = lambda n: pltpu.SemaphoreType.DMA((n,))
    scratch = (
        [half, half, half, vm(heads, T, F32), taps, taps, half]
        + [ext, ext] + [full] * 8 + [ext, ext]
        + [half] * 5 + [half, vm(T, BLOCK, BF16)]
        + [vm(nb * heads, BLOCK, F32), vm(nb * heads, BLOCK, F32), vm(3 * nb * heads, BLOCK, BF16)]
        + [vm(nb, 8, W, F32)]
        + [vm(nb, N, W, F32)] * 4
        + [vm(nb, N, W, BF16)] * 2
        + [vm(2, N, W, BF16), vm(nseq, N, W, BF16)]
        + [vm(2, 16, W + N, BF16), vm(nseq, 16, W + N, BF16)]
        + [vm(BLOCK, heads * BLOCK, BF16), vm(heads * BLOCK, W, BF16), vm(heads * BLOCK, W, BF16)]
        + [vm(16, W, BF16)] * 2 + [vm(2, 8, W, F32)] * 2
        + [vm(nzy, nc, own, W, BF16), vm(nzy, own, W, BF16)]
        + [vm(nzy, own, W, BF16)] * 2
        + [vm(nseq, 8, W, F32)] * 2 + [vm(2, 8, W, F32), vm(nzy, 8, W, F32)]
        + [dma(7)] + [dma(2)] * 2 + [dma(nseq)] * 4 + [dma(2)] * 2 + [dma(3)] * 2 + [dma(nzy)] * 2
        + [dma(nseq)] * 4 + [dma(1)] * 2 + [dma(nzy)] * 2
    )
    vspec = pl.BlockSpec(memory_space=pltpu.VMEM)
    sspec = pl.BlockSpec(memory_space=pltpu.SMEM)
    hspec = pl.BlockSpec(memory_space=pltpu.HBM)
    shapes = [
        ((T, W), BF16), ((T, W), BF16), ((heads, T), F32), ((own, W), F32), ((TAPS, W), F32), ((TAPS, W), F32),
    ]
    held = pl.pallas_call(
        functools.partial(kernel, dims, T, W),
        name="ssd_backward",
        out_shape=tuple(pltpu.VMEM(*sh) for sh in shapes),
        in_specs=[hspec, hspec, hspec, hspec, sspec, sspec, hspec, hspec, hspec],
        out_specs=tuple([vspec] * 6),
        scratch_shapes=scratch,
        compiler_params=pltpu.CompilerParams(
            collective_id=0, has_side_effects=True, vmem_limit_bytes=60 * 1024 * 1024
        ),
    )(xraw, zgate, bcraw, dt, a_rate, d_skip, conv_x, conv_bc, dout)
    return pl.pallas_call(
        emit,
        name="emit",
        out_shape=tuple(jax.ShapeDtypeStruct(*sh) for sh in shapes),
        in_specs=[vspec] * 6,
        out_specs=tuple([hspec] * 6),
        scratch_shapes=[dma(6)],
        compiler_params=pltpu.CompilerParams(vmem_limit_bytes=4 * 1024 * 1024),
    )(*held)


def over_mesh(torus):
    placed = (
        P(SEQ, HEAD), P(SEQ, HEAD), P(SEQ, None), P(HEAD, SEQ), P(HEAD), P(HEAD),
        P(None, HEAD), P(), P(SEQ, HEAD),
    )
    return jax.shard_map(
        functools.partial(local, tuple(torus.devices.shape)),
        mesh=torus,
        in_specs=placed,
        out_specs=(P(SEQ, HEAD), P(SEQ, HEAD), P(HEAD, SEQ), P(SEQ_HEAD, None), P(None, HEAD), P()),
        check_vma=False,
    )


def solution(mesh):
    return over_mesh(Mesh(mesh.devices.reshape(4, 2, 8, 2, 2), SEQ_HEAD))
```

```python
import functools

import jax
import jax.numpy as jnp
from jax import lax
from jax.experimental import pallas as pl
from jax.experimental.pallas import tpu as pltpu
from jax.sharding import Mesh
from jax.sharding import PartitionSpec as P

HEAD_DIM = 64
BLOCK = 256
TAPS = 4
SEQ = ("seq_0", "seq_1")
HEAD = ("head_0", "head_1", "head_2")
SEQ_HEAD = SEQ + HEAD
F32, BF16 = jnp.float32, jnp.bfloat16


def mm(a, b, dims=((1,), (0,))):
    return lax.dot_general(a, b, (dims, ((), ())), preferred_element_type=F32)


NT = ((1,), (1,))
TN = ((0,), (0,))


def parts3(v):
    p1 = v.astype(BF16)
    r1 = v - p1.astype(F32)
    p2 = r1.astype(BF16)
    r2 = r1 - p2.astype(F32)
    return p1, p2, r2.astype(BF16)


def sigmoid(v):
    return 0.5 * jnp.tanh(0.5 * v) + 0.5


def silu_slope(v):
    q = sigmoid(v)
    return q * (1.0 + v * (1.0 - q))


def loop(lo, hi, body, carry=0, unroll=1):
    if unroll >= hi - lo:
        for i in range(lo, hi):
            carry = body(i, carry)
        return carry

    def some(j, carry):
        for u in range(unroll):
            carry = body(lo + j * unroll + u, carry)
        return carry

    return lax.fori_loop(0, (hi - lo) // unroll, some, carry)


def part(k, n):
    return pl.ds(k * n if isinstance(k, int) else pl.multiple_of(k * n, n), n)


def window(start, n):
    return pl.ds(start if isinstance(start, int) else pl.multiple_of(start, 8), n)


def by_head(scalars, lanes):
    out = jnp.full(lanes.shape, scalars[3], F32)
    for h in (2, 1, 0):
        out = jnp.where(lanes == h, scalars[h], out)
    return out


def kernel(
    dims, T, W,
    xraw_h, zg_h, bcr_h, dt_h, a_s, d_s, cvx_h, cvb_h, dout_h,
    xg_o, gg_o, sg_o, bg_o, cx_o, cb_o,
    xraw, zg, bcr, dt, cvx, cvb, dout,
    XF, BCF, XS, BCS, DTE, ENT, LEA, YIN, WGIN, XSL, BS,
    XP, WX, WL, DY, DYE, BCP, MX,
    GC, DC, WP, TOT, LS, NS, SB, GB, EB, SLOT, CR, CSLOT, FS, DEC,
    KH, WXM, DYM, HXR, HBR, HSX, HSB,
    PR, RA, ZS, RZ, CXS, CBS, CBZ,
    s_in, s_h, r_h, s_st, r_st, s_cr, r_cr, s_sl, r_sl, s_a, r_a, s_z, r_z,
    s_cx, r_cx, s_cb, r_cb, s_cz, r_cz,
):
    nx, nyh, nz, nyl, nc = dims
    nseq = nx * nyh
    nzy = nz * nyl
    nb = T // BLOCK
    heads = W // HEAD_DIM
    own = T // (nzy * nc)
    sx, sy = lax.axis_index("seq_0"), lax.axis_index("seq_1")
    s = sx * nyh + sy
    z, yl, c = (lax.axis_index(n) for n in HEAD)
    m = z * nyl + yl

    def at_seq(p):
        return {"seq_0": p // nyh, "seq_1": lax.rem(p, nyh)}

    def at_zy(p):
        return {"head_0": p // nyl, "head_1": lax.rem(p, nyl)}

    def other(d):
        wrapped = (s + d) // nseq
        return s + d - nseq * wrapped, wrapped

    def other_zy(d):
        return lax.rem(m + d, nzy)

    far_first = sorted(range(1, nzy), key=lambda d: -min(d, nzy - d))

    def send(src, dst, ss, rs, dev):
        return pltpu.make_async_remote_copy(
            src_ref=src, dst_ref=dst, send_sem=ss, recv_sem=rs,
            device_id=dev, device_id_type=pl.DeviceIdType.MESH,
        )

    core_dev = {"head_2": 1 - c}

    barrier = pltpu.get_barrier_semaphore()

    def greet(dev):
        pl.semaphore_signal(barrier, inc=1, device_id=dev, device_id_type=pl.DeviceIdType.MESH)

    for d in range(1, nseq):
        greet(at_seq(other(d)[0]))
    for d in far_first:
        greet(at_zy(other_zy(d)))
    greet(core_dev)
    for d in range(1, nseq):
        greet({**at_seq(other(d)[0]), **core_dev})

    loads = [
        pltpu.make_async_copy(a, b, s_in.at[i])
        for i, (a, b) in enumerate(
            [(dt_h, dt), (zg_h, zg), (dout_h, dout), (bcr_h, bcr), (xraw_h, xraw),
             (cvx_h, cvx), (cvb_h, cvb)]
        )
    ]
    for load in loads:
        load.start()

    rows16 = lax.broadcasted_iota(jnp.int32, (heads, BLOCK), 0)
    a_col = by_head([a_s[h] for h in range(heads)], rows16)
    n16 = nb * heads
    ri = lax.broadcasted_iota(jnp.int32, (BLOCK, BLOCK), 0)
    ci = lax.broadcasted_iota(jnp.int32, (BLOCK, BLOCK), 1)
    tri = (ri <= ci).astype(F32).astype(BF16)
    rr = lax.rem(lax.broadcasted_iota(jnp.int32, (3 * n16, W), 0), n16)
    ll = lax.broadcasted_iota(jnp.int32, (3 * n16, W), 1) // HEAD_DIM
    loads[0].wait()
    for k in range(nb):
        piece = dt[:, k * BLOCK : (k + 1) * BLOCK]
        DC[k * heads : (k + 1) * heads, :] = piece
        GC[k * heads : (k + 1) * heads, :] = piece * a_col
    w3 = mm(jnp.concatenate(parts3(GC[...]), axis=0), tri)
    within = w3[:n16] + w3[n16 : 2 * n16] + w3[2 * n16 :]
    GC[...] = within
    wp = jnp.concatenate(parts3(within), axis=0)
    dp = jnp.concatenate(parts3(DC[...]), axis=0)
    WP[...] = wp

    def blk(k, n=BLOCK):
        return part(k, n)

    def expand(k, carry):
        hot = ((rr // heads == k) & (lax.rem(rr, heads) == ll)).astype(F32).astype(BF16)
        wexp = mm(wp, hot, TN)
        total = wexp[BLOCK - 1 : BLOCK, :]
        TOT[k] = jnp.broadcast_to(total, (8, W))
        ENT[blk(k), :] = jnp.exp(-wexp)
        LEA[blk(k), :] = jnp.exp(jnp.minimum(wexp - total, 0.0))
        DTE[blk(k), :] = mm(dp, hot, TN)
        return carry

    loop(0, nb, expand, 0, 2)

    CH = 64
    N = W // 2
    per = BLOCK // CH
    for load in loads[1:]:
        load.wait()
    XF[0:8, :] = jnp.zeros((8, W), F32)
    BCF[0:8, :] = jnp.zeros((8, W), F32)

    def gates(i, carry):
        r = blk(i, CH)
        zv = zg[r, :].astype(F32)
        dy = (dout[r, :].astype(F32) * (zv * sigmoid(zv))).astype(BF16)
        DY[r, :] = dy
        DYE[r, :] = (dy.astype(F32) * ENT[r, :]).astype(BF16)
        shifted = window(8 + i * CH, CH)
        XF[shifted, :] = xraw[r, :].astype(F32)
        BCF[shifted, :] = bcr[r, :].astype(F32)
        return carry

    loop(0, T // CH, gates, 0, 2)

    def pre(F, taps, i):
        v = F[window(i * CH, CH + 8), :]
        out = taps[0:1, :] * v[8:, :]
        for k in range(1, TAPS):
            out = out + taps[k : k + 1, :] * pltpu.roll(v, k, 0)[8:, :]
        return out

    def conv_bc_chunk(i, carry):
        v = pre(BCF, cvb, i)
        BCP[blk(i, CH), :] = (v * sigmoid(v)).astype(BF16)
        BCS[blk(i, CH), :] = v
        return carry

    def conv_x_chunk(i, carry):
        r = blk(i, CH)
        v = pre(XF, cvx, i)
        post = (v * sigmoid(v)).astype(BF16)
        XP[r, :] = post
        XS[r, :] = v
        wx = (post.astype(F32) * DTE[r, :]).astype(BF16)
        WX[r, :] = wx
        WL[r, :] = (wx.astype(F32) * LEA[r, :]).astype(BF16)
        return carry

    loop(0, T // CH, conv_bc_chunk, 0, 2)
    rt = lax.broadcasted_iota(jnp.int32, (16, W), 0)
    edge = rt < TAPS - 1
    BCP[0:16, :] = jnp.where(edge, jnp.zeros((16, W), BF16), BCP[0:16, :])

    grads = [mm(BCP[blk(k), N:], DYE[blk(k), :], TN) for k in range(nb)]
    grad = jnp.zeros((N, W), F32)
    for k in reversed(range(nb)):
        NS[k] = grad
        grad = jnp.exp(-TOT[k][0:1, :]) * grad + grads[k]
    EB[1] = grad.astype(BF16)

    pl.semaphore_wait(barrier, nseq * nc - 1 + nzy - 1)

    halo_x = send(xraw.at[T - 16 :], HXR, s_h.at[0], r_h.at[0], at_seq(s + 1))
    halo_b = send(bcr.at[T - 16 :], HBR, s_h.at[1], r_h.at[1], at_seq(s + 1))

    @pl.when(s < nseq - 1)
    def _():
        halo_x.start()
        halo_b.start()

    def state_copy(d):
        p, wrapped = other(d)
        return send(EB.at[wrapped], SLOT.at[s], s_st.at[d], r_st.at[s], at_seq(p))

    def edge_copy(d):
        p, wrapped = other(d)
        return send(CR.at[wrapped], CSLOT.at[s], s_cr.at[d], r_cr.at[s], at_seq(p))

    for d in sorted(range(1, nseq), key=lambda d: -min(d, nseq - d)):

        @pl.when(s + d >= nseq)
        def _():
            state_copy(d).start()

    loop(0, T // CH, conv_x_chunk, 0, 2)
    ends = [mm(BCP[blk(k), :N], WL[blk(k), :], TN) for k in range(nb)]
    state = jnp.zeros((N, W), F32)
    for k in range(nb):
        LS[k] = state
        state = jnp.exp(-TOT[k][0:1, :]) * state + ends[k]
    EB[0] = state.astype(BF16)
    for d in sorted(range(1, nseq), key=lambda d: -min(d, nseq - d)):

        @pl.when(s + d < nseq)
        def _():
            state_copy(d).start()

    lane_h = lax.broadcasted_iota(jnp.int32, (BLOCK, W), 1) // HEAD_DIM
    r512 = lax.rem(lax.broadcasted_iota(jnp.int32, (3 * n16, heads * 128), 0), n16)
    l512 = lax.broadcasted_iota(jnp.int32, (3 * n16, heads * 128), 1) // 128
    for h in range(heads):
        KH[:, 0:128, h * BLOCK + 128 : (h + 1) * BLOCK] = jnp.zeros((nb, 128, 128), BF16)
    TQ = 64

    def inside(k, carry):
        bm, cm = BCP[blk(k), :N], BCP[blk(k), N:]
        wx, dy = WX[blk(k), :], DY[blk(k), :]
        for h in range(heads):
            DYM[k, h * BLOCK : (h + 1) * BLOCK, :] = jnp.where(lane_h == h, dy, jnp.zeros_like(dy))
        hot = ((r512 // heads == k) & (lax.rem(r512, heads) == l512)).astype(F32).astype(BF16)
        col = mm(WP[...], hot, TN)
        for t0 in range(0, BLOCK, TQ):
            ext = 128 if t0 < 128 else BLOCK
            sc = mm(cm[t0 : t0 + TQ, :], bm[0:ext, :], NT)
            tt = t0 + lax.broadcasted_iota(jnp.int32, (TQ, ext), 0)
            ss = lax.broadcasted_iota(jnp.int32, (TQ, ext), 1)
            keep = tt >= ss
            total = None
            for h in range(heads):
                wrow = GC[pl.ds(k * heads + h, 1), :][:, 0:ext]
                wcol = col[t0 : t0 + TQ, h * 128 : (h + 1) * 128]
                if ext > 128:
                    wcol = jnp.concatenate([wcol, wcol], axis=1)
                decay = jnp.where(keep, jnp.exp(jnp.minimum(wrow - wcol, 0.0)), 0.0)
                KH[k, t0 : t0 + TQ, h * BLOCK : h * BLOCK + ext] = (sc * decay).astype(BF16)
                mixing = mm(DYM[k, h * BLOCK + t0 : h * BLOCK + t0 + TQ, :], wx[0:ext, :], NT)
                part = mixing * decay
                total = part if total is None else total + part
            rows = window(k * BLOCK + t0, TQ)
            MX[rows, 0:ext] = total.astype(BF16)
            if ext < BLOCK:
                MX[rows, ext:] = jnp.zeros((TQ, BLOCK - ext), BF16)
        return carry

    def inner(k, carry):
        wx = WX[blk(k), :]
        for h in range(heads):
            WXM[h * BLOCK : (h + 1) * BLOCK, :] = jnp.where(lane_h == h, wx, jnp.zeros_like(wx))
        acc = None
        for h in range(heads):
            part_h = mm(
                KH[k, :, h * BLOCK : (h + 1) * BLOCK], DYM[k, h * BLOCK : (h + 1) * BLOCK, :], TN
            )
            acc = part_h if acc is None else acc + part_h
        WGIN[blk(k), :] = acc
        YIN[blk(k), :] = mm(KH[k], WXM[...])
        return carry

    loop(nb - 1, nb, inside, 0, 1)

    @pl.when(s > 0)
    def _():
        halo_x.wait_recv()
        halo_b.wait_recv()
        XF[0:8, :] = HXR[8:16, :].astype(F32)
        BCF[0:8, :] = HBR[8:16, :].astype(F32)

    conv_bc_chunk(0, 0)
    conv_x_chunk(0, 0)
    dtot = TOT[0][0:1, :]
    for k in range(1, nb):
        dtot = dtot + TOT[k][0:1, :]
    tail0 = TOT[0][0:1, :]
    q1, q2, q3 = (p.astype(F32) for p in parts3(dtot))

    def edge_rows(v):
        v = jnp.where(edge, v, 0.0)
        v = jnp.where(rt == 8, q1, jnp.where(rt == 9, q2, jnp.where(rt == 10, q3, v)))
        return v.astype(BF16)

    CR[0, :, 0:W] = edge_rows(
        WX[0:16, :].astype(F32) * LEA[0:16, :] * jnp.exp(jnp.minimum(tail0 - dtot, 0.0))
    )
    CR[1, :, 0:W] = edge_rows(DYE[0:16, :].astype(F32))
    first = jnp.where(edge, BCP[0:16, :], jnp.zeros((16, W), BF16))
    CR[0, :, W:] = first[:, :N]
    CR[1, :, W:] = first[:, N:]
    for d in range(1, nseq):
        edge_copy(d).start()
    start0 = mm(first[:, :N], WL[0:16, :], TN)

    loop(0, nb - 1, inside, 0, 1)

    def mixed(k, carry):
        r = blk(k)
        mx = MX[r, :]
        BS[r, :N] = mm(mx, BCP[r, N:], TN)
        BS[r, N:] = mm(mx, BCP[r, :N])
        BCS[r, :] = silu_slope(BCS[r, :])
        return carry

    loop(0, nb, mixed, 0, 4)

    for d in range(1, nseq):
        p, _ = other(d)
        send(EB.at[0], SLOT.at[p], s_st.at[d], r_st.at[p], at_seq(p)).wait_recv()
        send(CR.at[0], CSLOT.at[p], s_cr.at[d], r_cr.at[p], at_seq(p)).wait_recv()

    for d in range(1, nseq):
        p, _ = other(d)
        rows = CSLOT[p, :, 0:W]
        t3 = rows[8:16, :].astype(F32)
        DEC[p] = jnp.broadcast_to(jnp.exp(-(t3[0:1, :] + t3[1:2, :] + t3[2:3, :])), (8, W))
        FS[p] = SLOT[p].astype(F32) + mm(CSLOT[p, :, W:], rows, TN)

    def fold(p, value):
        return DEC[p][0:1, :] * value + FS[p]

    zero_state = jnp.zeros((N, W), F32)
    s_first = lax.fori_loop(0, s, fold, zero_state)
    g_last = lax.fori_loop(0, nseq - 1 - s, lambda i, v: fold(nseq - 1 - i, v), zero_state)
    SB[0] = s_first.astype(BF16)
    s_next = jnp.exp(-TOT[0][0:1, :]) * s_first + start0
    before = jnp.zeros((1, W), F32)
    for k in range(1, nb):
        SB[k] = (LS[k] + jnp.exp(-before) * s_next).astype(BF16)
        before = before + TOT[k][0:1, :]
    after = jnp.zeros((1, W), F32)
    for k in reversed(range(nb)):
        GB[k] = (NS[k] + jnp.exp(-after) * g_last).astype(BF16)
        after = after + TOT[k][0:1, :]

    def shared(k, carry):
        r = blk(k)
        BS[r, :N] = (BS[r, :N] + mm(WL[r, :], GB[k], NT)) * BCS[r, :N]
        BS[r, N:] = (BS[r, N:] + mm(DYE[r, :], SB[k], NT)) * BCS[r, N:]
        return carry

    shared(0, 0)
    HSB[0] = BS[0:8, :]
    halo_bs = send(HSB.at[0], HSB.at[1], s_sl.at[0], r_sl.at[0], at_seq(s - 1))

    @pl.when(s > 0)
    def _():
        halo_bs.start()

    loop(1, nb, shared, 0, 3)

    def bc_adjoint(j, carry):
        u = BS[window(j * own, own + 8), :]
        out = cvb[0:1, :] * u[:own, :]
        for k in range(1, TAPS):
            out = out + cvb[k : k + 1, :] * pltpu.roll(u, own + 8 - k, 0)[:own, :]
        PR[j // nc, lax.rem(j, nc)] = out.astype(BF16)
        return carry

    pieces = [(0, nzy // 2), (nzy // 2, nzy - 1), (nzy - 1, nzy)]

    def a_copy(q):
        lo, hi = pieces[q]
        part = pl.ds(lo, hi - lo)
        return send(PR.at[part, 1 - c], RA.at[part], s_a.at[q], r_a.at[q], core_dev)

    def adjoint_piece(q):
        loop(pieces[q][0] * nc, pieces[q][1] * nc, bc_adjoint, 0, 2)
        a_copy(q).start()

    def pair_sum(i, carry):
        ZS[i] = (PR[i, c].astype(F32) + RA[i].astype(F32)).astype(BF16)
        return carry

    def z_copy(d):
        t = other_zy(d)
        return send(ZS.at[t], RZ.at[m], s_z.at[d], r_z.at[m], at_zy(t))

    def tap_sums(slope, F, start, carry):
        n = slope.shape[0]
        v = F[window(start, n + 8), :]
        out = []
        for k in range(TAPS):
            moved = v[8:, :] if k == 0 else pltpu.roll(v, k, 0)[8:, :]
            out.append(carry[k] + (slope * moved).reshape(n // 8, 8, W).sum(axis=0))
        return tuple(out)

    def stack_taps(sums):
        rt4 = lax.broadcasted_iota(jnp.int32, (TAPS, W), 0)
        out = jnp.zeros((TAPS, W), F32)
        for k in range(TAPS):
            out = jnp.where(rt4 == k, jnp.sum(sums[k], axis=0, keepdims=True), out)
        return out

    zero4 = tuple(jnp.zeros((8, W), F32) for _ in range(TAPS))
    sums = loop(
        0, T // CH, lambda i, cr: tap_sums(BS[blk(i, CH), :], BCF, i * CH, cr), zero4, 2
    )
    CBZ[m] = stack_taps(sums)

    def cz_copy(d):
        return send(CBZ.at[m], CBZ.at[m], s_cz.at[d], r_cz.at[m], at_zy(other_zy(d)))

    for d in far_first:
        cz_copy(d).start()

    adjoint_piece(0)
    adjoint_piece(1)

    def seq_copy(buf, d, ss, rs):
        p, _ = other(d)
        return send(buf.at[s], buf.at[s], ss.at[d], rs.at[s], at_seq(p))

    def seq_wait(buf, ss, rs):
        for d in range(1, nseq):
            p, _ = other(d)
            send(buf.at[p], buf.at[p], ss.at[d], rs.at[p], at_seq(p)).wait_recv()

    CW = 128
    lane1 = lax.broadcasted_iota(jnp.int32, (1, W), 1) // HEAD_DIM
    skip = by_head([d_s[h] for h in range(heads)], lane1)
    pick = (
        lax.broadcasted_iota(jnp.int32, (16, W), 0)
        == lax.broadcasted_iota(jnp.int32, (16, W), 1) // HEAD_DIM
    ).astype(F32).astype(BF16)

    def channels(i, carry):
        r = blk(i, CW)
        k = i // (BLOCK // CW)
        wg = WGIN[r, :] + LEA[r, :] * mm(BCP[r, :N], GB[k])
        xp = XP[r, :].astype(F32)
        slope = (DTE[r, :] * wg + skip * DY[r, :].astype(F32)) * silu_slope(XS[r, :])
        XSL[r, :] = slope
        prod = xp * wg
        hi = prod.astype(BF16)
        lo = (prod - hi.astype(F32)).astype(BF16)
        steps = mm(pick, hi, NT) + mm(pick, lo, NT)
        sg_o[:, part(i, CW)] = steps[0:heads, :]
        return tap_sums(slope, XF, i * CW, carry)

    halves = BLOCK // CW

    def block_channels(k, sums):
        inner(k, 0)
        return loop(k * halves, (k + 1) * halves, channels, sums, halves)

    sums = block_channels(0, zero4)
    HSX[0] = XSL[0:8, :]
    halo_xs = send(HSX.at[0], HSX.at[1], s_sl.at[1], r_sl.at[1], at_seq(s - 1))

    @pl.when(s > 0)
    def _():
        halo_xs.start()

    for q in range(2):
        a_copy(q).wait_recv()
        loop(pieces[q][0], pieces[q][1], pair_sum, 0, nzy)
    for d in far_first:

        @pl.when(other_zy(d) < nzy - 1)
        def _():
            z_copy(d).start()

    @pl.when(s < nseq - 1)
    def _():
        halo_bs.wait_recv()
        BS[T : T + 8, :] = HSB[1]

    @pl.when(s == nseq - 1)
    def _():
        BS[T : T + 8, :] = jnp.zeros((8, W), F32)

    adjoint_piece(2)
    sums = block_channels(1, sums)
    a_copy(2).wait_recv()
    pair_sum(nzy - 1, 0)

    @pl.when(m < nzy - 1)
    def _():
        z_copy(nzy - 1 - m).start()

    sums = block_channels(2, sums)
    sums = block_channels(3, sums)
    CXS[s] = stack_taps(sums)
    for d in range(1, nseq):
        seq_copy(CXS, d, s_cx, r_cx).start()

    def total(buf, n):
        out = buf[0]
        for p in range(1, n):
            out = out + buf[p]
        return out

    for d in range(1, nzy):
        t = other_zy(d)
        send(CBZ.at[t], CBZ.at[t], s_cz.at[d], r_cz.at[t], at_zy(t)).wait_recv()
    mine = s * nc + c
    CBS[mine] = total(CBZ, nzy)

    def sc_copy(d):
        p, _ = other(d // 2)
        dev = at_seq(p) if d % 2 == 0 else {**at_seq(p), **core_dev}
        return send(CBS.at[mine], CBS.at[mine], s_cb.at[d], r_cb.at[mine], dev)

    for d in range(1, nseq * nc):
        sc_copy(d).start()

    def outputs(i, carry):
        r = blk(i, CH)
        k = i // (BLOCK // CH)
        y = YIN[r, :] + ENT[r, :] * mm(BCP[r, N:], SB[k]) + skip * XP[r, :].astype(F32)
        gate = dout[r, :].astype(F32) * silu_slope(zg[r, :].astype(F32))
        gg_o[r, :] = (gate * y).astype(BF16)
        return carry

    loop(0, T // CH, outputs, 0, 4)

    def x_adjoint(i, carry):
        r = blk(i, CH)
        u = XSL[window(i * CH, CH + 8), :]
        out = cvx[0:1, :] * u[:CH, :]
        for k in range(1, TAPS):
            out = out + cvx[k : k + 1, :] * pltpu.roll(u, CH + 8 - k, 0)[:CH, :]
        xg_o[r, :] = out.astype(BF16)
        return carry

    @pl.when(s < nseq - 1)
    def _():
        halo_xs.wait_recv()
        XSL[T : T + 8, :] = HSX[1]

    @pl.when(s == nseq - 1)
    def _():
        XSL[T : T + 8, :] = jnp.zeros((8, W), F32)

    loop(0, T // CH, x_adjoint, 0, 2)

    seq_wait(CXS, s_cx, r_cx)
    cx_o[...] = total(CXS, nseq)
    out = PR[m, c].astype(F32) + RA[m].astype(F32)
    for d in range(1, nzy):
        t = other_zy(d)
        send(ZS.at[t], RZ.at[t], s_z.at[d], r_z.at[t], at_zy(t)).wait_recv()
        out = out + RZ[t].astype(F32)
    bg_o[...] = out
    for d in range(1, nseq * nc):
        p, _ = other(d // 2)
        slot = p * nc + (c if d % 2 == 0 else 1 - c)
        send(CBS.at[slot], CBS.at[slot], s_cb.at[d], r_cb.at[slot], core_dev).wait_recv()
    cb_o[...] = total(CBS, nseq * nc)

    @pl.when(s < nseq - 1)
    def _():
        halo_x.wait_send()
        halo_b.wait_send()

    @pl.when(s > 0)
    def _():
        halo_bs.wait_send()
        halo_xs.wait_send()

    for d in range(1, nseq):
        state_copy(d).wait_send()
        edge_copy(d).wait_send()
        seq_copy(CXS, d, s_cx, r_cx).wait_send()
    for q in range(3):
        a_copy(q).wait_send()
    for d in range(1, nzy):
        z_copy(d).wait_send()
        cz_copy(d).wait_send()
    for d in range(1, nseq * nc):
        sc_copy(d).wait_send()


def emit(*refs):
    held, outs, sem = refs[:6], refs[6:12], refs[12]
    copies = [pltpu.make_async_copy(a, b, sem.at[i]) for i, (a, b) in enumerate(zip(held, outs))]
    for copy in copies:
        copy.start()
    for copy in copies:
        copy.wait()


def local(dims, xraw, zgate, bcraw, dt, a_rate, d_skip, conv_x, conv_bc, dout):
    nx, nyh, nz, nyl, nc = dims
    nseq = nx * nyh
    nzy = nz * nyl
    T, W = xraw.shape
    nb = T // BLOCK
    heads = W // HEAD_DIM
    N = W // 2
    own = T // (nzy * nc)
    vm = lambda *shape: pltpu.VMEM(shape[:-1], shape[-1])
    full, half = vm(T, W, F32), vm(T, W, BF16)
    ext = vm(T + 8, W, F32)
    taps = vm(TAPS, W, F32)
    dma = lambda n: pltpu.SemaphoreType.DMA((n,))
    scratch = (
        [half, half, half, vm(heads, T, F32), taps, taps, half]
        + [ext, ext] + [full] * 7 + [ext, ext]
        + [half] * 5 + [half, vm(T, BLOCK, BF16)]
        + [vm(nb * heads, BLOCK, F32), vm(nb * heads, BLOCK, F32), vm(3 * nb * heads, BLOCK, BF16)]
        + [vm(nb, 8, W, F32)]
        + [vm(nb, N, W, F32)] * 2
        + [vm(nb, N, W, BF16)] * 2
        + [vm(2, N, W, BF16), vm(nseq, N, W, BF16)]
        + [vm(2, 16, W + N, BF16), vm(nseq, 16, W + N, BF16)]
        + [vm(nseq, N, W, F32), vm(nseq, 8, W, F32)]
        + [vm(nb, BLOCK, heads * BLOCK, BF16), vm(heads * BLOCK, W, BF16)]
        + [vm(nb, heads * BLOCK, W, BF16)]
        + [vm(16, W, BF16)] * 2 + [vm(2, 8, W, F32)] * 2
        + [vm(nzy, nc, own, W, BF16), vm(nzy, own, W, BF16)]
        + [vm(nzy, own, W, BF16)] * 2
        + [vm(nseq, TAPS, W, F32), vm(nseq * nc, TAPS, W, F32), vm(nzy, TAPS, W, F32)]
        + [dma(7)] + [dma(2)] * 2 + [dma(nseq)] * 4 + [dma(2)] * 2 + [dma(3)] * 2 + [dma(nzy)] * 2
        + [dma(nseq)] * 2 + [dma(nseq * nc)] * 2 + [dma(nzy)] * 2
    )
    vspec = pl.BlockSpec(memory_space=pltpu.VMEM)
    sspec = pl.BlockSpec(memory_space=pltpu.SMEM)
    hspec = pl.BlockSpec(memory_space=pltpu.HBM)
    shapes = [
        ((T, W), BF16), ((T, W), BF16), ((heads, T), F32), ((own, W), F32), ((TAPS, W), F32), ((TAPS, W), F32),
    ]
    held = pl.pallas_call(
        functools.partial(kernel, dims, T, W),
        name="ssd_backward",
        out_shape=tuple(pltpu.VMEM(*sh) for sh in shapes),
        in_specs=[hspec, hspec, hspec, hspec, sspec, sspec, hspec, hspec, hspec],
        out_specs=tuple([vspec] * 6),
        scratch_shapes=scratch,
        compiler_params=pltpu.CompilerParams(
            collective_id=0, has_side_effects=True, vmem_limit_bytes=60 * 1024 * 1024
        ),
    )(xraw, zgate, bcraw, dt, a_rate, d_skip, conv_x, conv_bc, dout)
    return pl.pallas_call(
        emit,
        name="emit",
        out_shape=tuple(jax.ShapeDtypeStruct(*sh) for sh in shapes),
        in_specs=[vspec] * 6,
        out_specs=tuple([hspec] * 6),
        scratch_shapes=[dma(6)],
        compiler_params=pltpu.CompilerParams(vmem_limit_bytes=4 * 1024 * 1024),
    )(*held)


def over_mesh(torus):
    placed = (
        P(SEQ, HEAD), P(SEQ, HEAD), P(SEQ, None), P(HEAD, SEQ), P(HEAD), P(HEAD),
        P(None, HEAD), P(), P(SEQ, HEAD),
    )
    return jax.shard_map(
        functools.partial(local, tuple(torus.devices.shape)),
        mesh=torus,
        in_specs=placed,
        out_specs=(P(SEQ, HEAD), P(SEQ, HEAD), P(HEAD, SEQ), P(SEQ_HEAD, None), P(None, HEAD), P()),
        check_vma=False,
    )


def solution(mesh):
    return over_mesh(Mesh(mesh.devices.reshape(4, 2, 8, 2, 2), SEQ_HEAD))
```

```python
import functools

import jax
import jax.numpy as jnp
from jax import lax
from jax.experimental import pallas as pl
from jax.experimental.pallas import tpu as pltpu
from jax.sharding import Mesh
from jax.sharding import PartitionSpec as P

HEAD_DIM = 64
BLOCK = 256
TAPS = 4
SEQ = ("seq_0", "seq_1")
HEAD = ("head_0", "head_1", "head_2")
SEQ_HEAD = SEQ + HEAD
F32, BF16 = jnp.float32, jnp.bfloat16


def mm(a, b, dims=((1,), (0,))):
    return lax.dot_general(a, b, (dims, ((), ())), preferred_element_type=F32)


NT = ((1,), (1,))
TN = ((0,), (0,))


def parts3(v):
    p1 = v.astype(BF16)
    r1 = v - p1.astype(F32)
    p2 = r1.astype(BF16)
    r2 = r1 - p2.astype(F32)
    return p1, p2, r2.astype(BF16)


def sigmoid(v):
    return 0.5 * jnp.tanh(0.5 * v) + 0.5


def silu_slope(v):
    q = sigmoid(v)
    return q * (1.0 + v * (1.0 - q))


def loop(lo, hi, body, carry=0, unroll=1):
    if unroll >= hi - lo:
        for i in range(lo, hi):
            carry = body(i, carry)
        return carry

    def some(j, carry):
        for u in range(unroll):
            carry = body(lo + j * unroll + u, carry)
        return carry

    return lax.fori_loop(0, (hi - lo) // unroll, some, carry)


def part(k, n):
    return pl.ds(k * n if isinstance(k, int) else pl.multiple_of(k * n, n), n)


def window(start, n):
    return pl.ds(start if isinstance(start, int) else pl.multiple_of(start, 8), n)


def by_head(scalars, lanes):
    out = jnp.full(lanes.shape, scalars[3], F32)
    for h in (2, 1, 0):
        out = jnp.where(lanes == h, scalars[h], out)
    return out


def kernel(
    dims, T, W,
    xraw_h, zg_h, bcr_h, dt_h, a_h, d_h, cvx_h, cvb_h, dout_h,
    xg_o, gg_o, sg_o, bg_o, cx_o, cb_o,
    xraw, zg, bcr, dt, cvx, cvb, dout, a_s, d_s,
    XF, BCF, XS, BCS, DTE, ENT, LEA, YIN, WGIN, XSL, BS,
    XP, WX, WL, DY, DYE, BCP, MX,
    GC, DC, WP, TOT, LS, NS, SB, GB, EB, SLOT, CR, CSLOT, FS, DEC,
    KH, WXM, DYM, HXR, HBR, HSX, HSB,
    PR, RA, ZS, RZ, CXS, CBS, CBZ,
    s_in, s_h, r_h, s_st, r_st, s_cr, r_cr, s_sl, r_sl, s_a, r_a, s_z, r_z,
    s_cx, r_cx, s_cb, r_cb, s_cz, r_cz,
):
    nx, nyh, nz, nyl, nc = dims
    nseq = nx * nyh
    nzy = nz * nyl
    nb = T // BLOCK
    heads = W // HEAD_DIM
    own = T // (nzy * nc)
    sx, sy = lax.axis_index("seq_0"), lax.axis_index("seq_1")
    s = sx * nyh + sy
    z, yl, c = (lax.axis_index(n) for n in HEAD)
    m = z * nyl + yl

    def at_seq(p):
        return {"seq_0": p // nyh, "seq_1": lax.rem(p, nyh)}

    def at_zy(p):
        return {"head_0": p // nyl, "head_1": lax.rem(p, nyl)}

    def other(d):
        wrapped = (s + d) // nseq
        return s + d - nseq * wrapped, wrapped

    def other_zy(d):
        return lax.rem(m + d, nzy)

    far_first = sorted(range(1, nzy), key=lambda d: -min(d, nzy - d))

    def send(src, dst, ss, rs, dev):
        return pltpu.make_async_remote_copy(
            src_ref=src, dst_ref=dst, send_sem=ss, recv_sem=rs,
            device_id=dev, device_id_type=pl.DeviceIdType.MESH,
        )

    core_dev = {"head_2": 1 - c}

    barrier = pltpu.get_barrier_semaphore()

    def greet(dev):
        pl.semaphore_signal(barrier, inc=1, device_id=dev, device_id_type=pl.DeviceIdType.MESH)

    for d in range(1, nseq):
        greet(at_seq(other(d)[0]))
    for d in far_first:
        greet(at_zy(other_zy(d)))
    greet(core_dev)
    for d in range(1, nseq):
        greet({**at_seq(other(d)[0]), **core_dev})

    loads = [
        pltpu.make_async_copy(a, b, s_in.at[i])
        for i, (a, b) in enumerate(
            [(dt_h, dt), (a_h, a_s), (d_h, d_s), (cvb_h, cvb), (cvx_h, cvx),
             (dout_h, dout), (zg_h, zg), (bcr_h, bcr), (xraw_h, xraw)]
        )
    ]
    for load in loads:
        load.start()

    rows16 = lax.broadcasted_iota(jnp.int32, (heads, BLOCK), 0)
    n16 = nb * heads
    ri = lax.broadcasted_iota(jnp.int32, (BLOCK, BLOCK), 0)
    ci = lax.broadcasted_iota(jnp.int32, (BLOCK, BLOCK), 1)
    tri = (ri <= ci).astype(F32).astype(BF16)
    rr = lax.rem(lax.broadcasted_iota(jnp.int32, (3 * n16, W), 0), n16)
    ll = lax.broadcasted_iota(jnp.int32, (3 * n16, W), 1) // HEAD_DIM
    for load in loads[:3]:
        load.wait()
    a_col = by_head([a_s[h] for h in range(heads)], rows16)
    for k in range(nb):
        piece = dt[:, k * BLOCK : (k + 1) * BLOCK]
        DC[k * heads : (k + 1) * heads, :] = piece
        GC[k * heads : (k + 1) * heads, :] = piece * a_col
    w3 = mm(jnp.concatenate(parts3(GC[...]), axis=0), tri)
    within = w3[:n16] + w3[n16 : 2 * n16] + w3[2 * n16 :]
    GC[...] = within
    wp = jnp.concatenate(parts3(within), axis=0)
    dp = jnp.concatenate(parts3(DC[...]), axis=0)
    WP[...] = wp

    def blk(k, n=BLOCK):
        return part(k, n)

    def expand(k, carry):
        hot = ((rr // heads == k) & (lax.rem(rr, heads) == ll)).astype(F32).astype(BF16)
        wexp = mm(wp, hot, TN)
        total = wexp[BLOCK - 1 : BLOCK, :]
        TOT[k] = jnp.broadcast_to(total, (8, W))
        ENT[blk(k), :] = jnp.exp(-wexp)
        LEA[blk(k), :] = jnp.exp(jnp.minimum(wexp - total, 0.0))
        DTE[blk(k), :] = mm(dp, hot, TN)
        return carry

    loop(0, nb, expand, 0, 2)

    CH = 64
    N = W // 2
    per = BLOCK // CH
    for load in loads[3:8]:
        load.wait()
    XF[0:8, :] = jnp.zeros((8, W), F32)
    BCF[0:8, :] = jnp.zeros((8, W), F32)

    def gates(i, carry):
        r = blk(i, CH)
        zv = zg[r, :].astype(F32)
        dy = (dout[r, :].astype(F32) * (zv * sigmoid(zv))).astype(BF16)
        DY[r, :] = dy
        DYE[r, :] = (dy.astype(F32) * ENT[r, :]).astype(BF16)
        shifted = window(8 + i * CH, CH)
        BCF[shifted, :] = bcr[r, :].astype(F32)
        return carry

    loop(0, T // CH, gates, 0, 2)

    def pre(F, taps, i):
        v = F[window(i * CH, CH + 8), :]
        out = taps[0:1, :] * v[8:, :]
        for k in range(1, TAPS):
            out = out + taps[k : k + 1, :] * pltpu.roll(v, k, 0)[8:, :]
        return out

    def conv_bc_chunk(i, carry):
        v = pre(BCF, cvb, i)
        BCP[blk(i, CH), :] = (v * sigmoid(v)).astype(BF16)
        BCS[blk(i, CH), :] = v
        return carry

    def conv_x_chunk(i, carry):
        r = blk(i, CH)
        v = pre(XF, cvx, i)
        post = (v * sigmoid(v)).astype(BF16)
        XP[r, :] = post
        XS[r, :] = v
        wx = (post.astype(F32) * DTE[r, :]).astype(BF16)
        WX[r, :] = wx
        WL[r, :] = (wx.astype(F32) * LEA[r, :]).astype(BF16)
        return carry

    loop(0, T // CH, conv_bc_chunk, 0, 2)
    rt = lax.broadcasted_iota(jnp.int32, (16, W), 0)
    edge = rt < TAPS - 1
    BCP[0:16, :] = jnp.where(edge, jnp.zeros((16, W), BF16), BCP[0:16, :])

    grads = [mm(BCP[blk(k), N:], DYE[blk(k), :], TN) for k in range(nb)]
    grad = jnp.zeros((N, W), F32)
    for k in reversed(range(nb)):
        NS[k] = grad
        grad = jnp.exp(-TOT[k][0:1, :]) * grad + grads[k]
    EB[1] = grad.astype(BF16)

    pl.semaphore_wait(barrier, nseq * nc - 1 + nzy - 1)

    loads[8].wait()
    halo_x = send(xraw.at[T - 16 :], HXR, s_h.at[0], r_h.at[0], at_seq(s + 1))
    halo_b = send(bcr.at[T - 16 :], HBR, s_h.at[1], r_h.at[1], at_seq(s + 1))

    @pl.when(s < nseq - 1)
    def _():
        halo_x.start()
        halo_b.start()

    def state_copy(d):
        p, wrapped = other(d)
        return send(EB.at[wrapped], SLOT.at[s], s_st.at[d], r_st.at[s], at_seq(p))

    def edge_copy(d):
        p, wrapped = other(d)
        return send(CR.at[wrapped], CSLOT.at[s], s_cr.at[d], r_cr.at[s], at_seq(p))

    for d in sorted(range(1, nseq), key=lambda d: -min(d, nseq - d)):

        @pl.when(s + d >= nseq)
        def _():
            state_copy(d).start()

    def widen(i, carry):
        XF[window(8 + i * CH, CH), :] = xraw[blk(i, CH), :].astype(F32)
        return conv_x_chunk(i, carry)

    loop(0, T // CH, widen, 0, 2)
    ends = [mm(BCP[blk(k), :N], WL[blk(k), :], TN) for k in range(nb)]
    state = jnp.zeros((N, W), F32)
    for k in range(nb):
        LS[k] = state
        state = jnp.exp(-TOT[k][0:1, :]) * state + ends[k]
    EB[0] = state.astype(BF16)
    for d in sorted(range(1, nseq), key=lambda d: -min(d, nseq - d)):

        @pl.when(s + d < nseq)
        def _():
            state_copy(d).start()

    lane_h = lax.broadcasted_iota(jnp.int32, (BLOCK, W), 1) // HEAD_DIM
    r512 = lax.rem(lax.broadcasted_iota(jnp.int32, (3 * n16, heads * 128), 0), n16)
    l512 = lax.broadcasted_iota(jnp.int32, (3 * n16, heads * 128), 1) // 128
    for h in range(heads):
        KH[:, 0:128, h * BLOCK + 128 : (h + 1) * BLOCK] = jnp.zeros((nb, 128, 128), BF16)
    TQ = 64

    def inside(k, carry):
        bm, cm = BCP[blk(k), :N], BCP[blk(k), N:]
        wx, dy = WX[blk(k), :], DY[blk(k), :]
        for h in range(heads):
            DYM[k, h * BLOCK : (h + 1) * BLOCK, :] = jnp.where(lane_h == h, dy, jnp.zeros_like(dy))
        hot = ((r512 // heads == k) & (lax.rem(r512, heads) == l512)).astype(F32).astype(BF16)
        col = mm(WP[...], hot, TN)
        for t0 in range(0, BLOCK, TQ):
            ext = 128 if t0 < 128 else BLOCK
            sc = mm(cm[t0 : t0 + TQ, :], bm[0:ext, :], NT)
            tt = t0 + lax.broadcasted_iota(jnp.int32, (TQ, ext), 0)
            ss = lax.broadcasted_iota(jnp.int32, (TQ, ext), 1)
            keep = tt >= ss
            total = None
            for h in range(heads):
                wrow = GC[pl.ds(k * heads + h, 1), :][:, 0:ext]
                wcol = col[t0 : t0 + TQ, h * 128 : (h + 1) * 128]
                if ext > 128:
                    wcol = jnp.concatenate([wcol, wcol], axis=1)
                decay = jnp.where(keep, jnp.exp(jnp.minimum(wrow - wcol, 0.0)), 0.0)
                KH[k, t0 : t0 + TQ, h * BLOCK : h * BLOCK + ext] = (sc * decay).astype(BF16)
                mixing = mm(DYM[k, h * BLOCK + t0 : h * BLOCK + t0 + TQ, :], wx[0:ext, :], NT)
                part = mixing * decay
                total = part if total is None else total + part
            rows = window(k * BLOCK + t0, TQ)
            MX[rows, 0:ext] = total.astype(BF16)
            if ext < BLOCK:
                MX[rows, ext:] = jnp.zeros((TQ, BLOCK - ext), BF16)
        return carry

    def inner(k, carry):
        wx = WX[blk(k), :]
        for h in range(heads):
            WXM[h * BLOCK : (h + 1) * BLOCK, :] = jnp.where(lane_h == h, wx, jnp.zeros_like(wx))
        acc = None
        for h in range(heads):
            part_h = mm(
                KH[k, :, h * BLOCK : (h + 1) * BLOCK], DYM[k, h * BLOCK : (h + 1) * BLOCK, :], TN
            )
            acc = part_h if acc is None else acc + part_h
        WGIN[blk(k), :] = acc
        YIN[blk(k), :] = mm(KH[k], WXM[...])
        return carry

    loop(nb - 1, nb, inside, 0, 1)

    @pl.when(s > 0)
    def _():
        halo_x.wait_recv()
        halo_b.wait_recv()
        XF[0:8, :] = HXR[8:16, :].astype(F32)
        BCF[0:8, :] = HBR[8:16, :].astype(F32)

    conv_bc_chunk(0, 0)
    conv_x_chunk(0, 0)
    dtot = TOT[0][0:1, :]
    for k in range(1, nb):
        dtot = dtot + TOT[k][0:1, :]
    tail0 = TOT[0][0:1, :]
    q1, q2, q3 = (p.astype(F32) for p in parts3(dtot))

    def edge_rows(v):
        v = jnp.where(edge, v, 0.0)
        v = jnp.where(rt == 8, q1, jnp.where(rt == 9, q2, jnp.where(rt == 10, q3, v)))
        return v.astype(BF16)

    CR[0, :, 0:W] = edge_rows(
        WX[0:16, :].astype(F32) * LEA[0:16, :] * jnp.exp(jnp.minimum(tail0 - dtot, 0.0))
    )
    CR[1, :, 0:W] = edge_rows(DYE[0:16, :].astype(F32))
    first = jnp.where(edge, BCP[0:16, :], jnp.zeros((16, W), BF16))
    CR[0, :, W:] = first[:, :N]
    CR[1, :, W:] = first[:, N:]
    for d in range(1, nseq):
        edge_copy(d).start()
    start0 = mm(first[:, :N], WL[0:16, :], TN)

    loop(0, nb - 1, inside, 0, 1)

    def mixed(k, carry):
        r = blk(k)
        mx = MX[r, :]
        BS[r, :N] = mm(mx, BCP[r, N:], TN)
        BS[r, N:] = mm(mx, BCP[r, :N])
        BCS[r, :] = silu_slope(BCS[r, :])
        return carry

    loop(0, nb, mixed, 0, 4)

    for d in range(1, nseq):
        p, _ = other(d)
        send(EB.at[0], SLOT.at[p], s_st.at[d], r_st.at[p], at_seq(p)).wait_recv()
        send(CR.at[0], CSLOT.at[p], s_cr.at[d], r_cr.at[p], at_seq(p)).wait_recv()

    for d in range(1, nseq):
        p, _ = other(d)
        rows = CSLOT[p, :, 0:W]
        t3 = rows[8:16, :].astype(F32)
        DEC[p] = jnp.broadcast_to(jnp.exp(-(t3[0:1, :] + t3[1:2, :] + t3[2:3, :])), (8, W))
        FS[p] = SLOT[p].astype(F32) + mm(CSLOT[p, :, W:], rows, TN)

    def fold(p, value):
        return DEC[p][0:1, :] * value + FS[p]

    zero_state = jnp.zeros((N, W), F32)
    s_first = lax.fori_loop(0, s, fold, zero_state)
    g_last = lax.fori_loop(0, nseq - 1 - s, lambda i, v: fold(nseq - 1 - i, v), zero_state)
    SB[0] = s_first.astype(BF16)
    s_next = jnp.exp(-TOT[0][0:1, :]) * s_first + start0
    before = jnp.zeros((1, W), F32)
    for k in range(1, nb):
        SB[k] = (LS[k] + jnp.exp(-before) * s_next).astype(BF16)
        before = before + TOT[k][0:1, :]
    after = jnp.zeros((1, W), F32)
    for k in reversed(range(nb)):
        GB[k] = (NS[k] + jnp.exp(-after) * g_last).astype(BF16)
        after = after + TOT[k][0:1, :]

    def shared(k, carry):
        r = blk(k)
        BS[r, :N] = (BS[r, :N] + mm(WL[r, :], GB[k], NT)) * BCS[r, :N]
        BS[r, N:] = (BS[r, N:] + mm(DYE[r, :], SB[k], NT)) * BCS[r, N:]
        return carry

    shared(0, 0)
    HSB[0] = BS[0:8, :]
    halo_bs = send(HSB.at[0], HSB.at[1], s_sl.at[0], r_sl.at[0], at_seq(s - 1))

    @pl.when(s > 0)
    def _():
        halo_bs.start()

    loop(1, nb, shared, 0, 3)

    def bc_adjoint(j, carry):
        u = BS[window(j * own, own + 8), :]
        out = cvb[0:1, :] * u[:own, :]
        for k in range(1, TAPS):
            out = out + cvb[k : k + 1, :] * pltpu.roll(u, own + 8 - k, 0)[:own, :]
        PR[j // nc, lax.rem(j, nc)] = out.astype(BF16)
        return carry

    pieces = [(0, nzy // 2), (nzy // 2, nzy - 1), (nzy - 1, nzy)]

    def a_copy(q):
        lo, hi = pieces[q]
        part = pl.ds(lo, hi - lo)
        return send(PR.at[part, 1 - c], RA.at[part], s_a.at[q], r_a.at[q], core_dev)

    def adjoint_piece(q):
        loop(pieces[q][0] * nc, pieces[q][1] * nc, bc_adjoint, 0, 2)
        a_copy(q).start()

    def pair_sum(i, carry):
        ZS[i] = (PR[i, c].astype(F32) + RA[i].astype(F32)).astype(BF16)
        return carry

    def z_copy(d):
        t = other_zy(d)
        return send(ZS.at[t], RZ.at[m], s_z.at[d], r_z.at[m], at_zy(t))

    def tap_sums(slope, F, start, carry):
        n = slope.shape[0]
        v = F[window(start, n + 8), :]
        out = []
        for k in range(TAPS):
            moved = v[8:, :] if k == 0 else pltpu.roll(v, k, 0)[8:, :]
            out.append(carry[k] + (slope * moved).reshape(n // 8, 8, W).sum(axis=0))
        return tuple(out)

    def stack_taps(sums):
        rt4 = lax.broadcasted_iota(jnp.int32, (TAPS, W), 0)
        out = jnp.zeros((TAPS, W), F32)
        for k in range(TAPS):
            out = jnp.where(rt4 == k, jnp.sum(sums[k], axis=0, keepdims=True), out)
        return out

    zero4 = tuple(jnp.zeros((8, W), F32) for _ in range(TAPS))
    sums = loop(
        0, T // CH, lambda i, cr: tap_sums(BS[blk(i, CH), :], BCF, i * CH, cr), zero4, 2
    )
    CBZ[m] = stack_taps(sums)

    def cz_copy(d):
        return send(CBZ.at[m], CBZ.at[m], s_cz.at[d], r_cz.at[m], at_zy(other_zy(d)))

    for d in far_first:
        cz_copy(d).start()

    adjoint_piece(0)
    adjoint_piece(1)

    def seq_copy(buf, d, ss, rs):
        p, _ = other(d)
        return send(buf.at[s], buf.at[s], ss.at[d], rs.at[s], at_seq(p))

    def seq_wait(buf, ss, rs):
        for d in range(1, nseq):
            p, _ = other(d)
            send(buf.at[p], buf.at[p], ss.at[d], rs.at[p], at_seq(p)).wait_recv()

    CW = 128
    lane1 = lax.broadcasted_iota(jnp.int32, (1, W), 1) // HEAD_DIM
    skip = by_head([d_s[h] for h in range(heads)], lane1)
    pick = (
        lax.broadcasted_iota(jnp.int32, (16, W), 0)
        == lax.broadcasted_iota(jnp.int32, (16, W), 1) // HEAD_DIM
    ).astype(F32).astype(BF16)

    def channels(i, carry):
        r = blk(i, CW)
        k = i // (BLOCK // CW)
        wg = WGIN[r, :] + LEA[r, :] * mm(BCP[r, :N], GB[k])
        xp = XP[r, :].astype(F32)
        slope = (DTE[r, :] * wg + skip * DY[r, :].astype(F32)) * silu_slope(XS[r, :])
        XSL[r, :] = slope
        prod = xp * wg
        hi = prod.astype(BF16)
        lo = (prod - hi.astype(F32)).astype(BF16)
        steps = mm(pick, hi, NT) + mm(pick, lo, NT)
        sg_o[:, part(i, CW)] = steps[0:heads, :]
        return tap_sums(slope, XF, i * CW, carry)

    halves = BLOCK // CW

    def block_channels(k, sums):
        inner(k, 0)
        return loop(k * halves, (k + 1) * halves, channels, sums, halves)

    sums = block_channels(0, zero4)
    HSX[0] = XSL[0:8, :]
    halo_xs = send(HSX.at[0], HSX.at[1], s_sl.at[1], r_sl.at[1], at_seq(s - 1))

    @pl.when(s > 0)
    def _():
        halo_xs.start()

    for q in range(2):
        a_copy(q).wait_recv()
        loop(pieces[q][0], pieces[q][1], pair_sum, 0, nzy)
    for d in far_first:

        @pl.when(other_zy(d) < nzy - 1)
        def _():
            z_copy(d).start()

    sums = block_channels(1, sums)
    sums = block_channels(2, sums)
    sums = block_channels(3, sums)
    CXS[s] = stack_taps(sums)
    for d in range(1, nseq):
        seq_copy(CXS, d, s_cx, r_cx).start()

    def total(buf, n):
        out = buf[0]
        for p in range(1, n):
            out = out + buf[p]
        return out

    def outputs(i, carry):
        r = blk(i, CH)
        k = i // (BLOCK // CH)
        y = YIN[r, :] + ENT[r, :] * mm(BCP[r, N:], SB[k]) + skip * XP[r, :].astype(F32)
        gate = dout[r, :].astype(F32) * silu_slope(zg[r, :].astype(F32))
        gg_o[r, :] = (gate * y).astype(BF16)
        return carry

    @pl.when(s < nseq - 1)
    def _():
        halo_bs.wait_recv()
        BS[T : T + 8, :] = HSB[1]

    @pl.when(s == nseq - 1)
    def _():
        BS[T : T + 8, :] = jnp.zeros((8, W), F32)

    adjoint_piece(2)
    loop(0, T // CH // 2, outputs, 0, 4)
    for d in range(1, nzy):
        t = other_zy(d)
        send(CBZ.at[t], CBZ.at[t], s_cz.at[d], r_cz.at[t], at_zy(t)).wait_recv()
    mine = s * nc + c
    CBS[mine] = total(CBZ, nzy)

    def sc_copy(d):
        p, _ = other(d // 2)
        dev = at_seq(p) if d % 2 == 0 else {**at_seq(p), **core_dev}
        return send(CBS.at[mine], CBS.at[mine], s_cb.at[d], r_cb.at[mine], dev)

    for d in range(1, nseq * nc):
        sc_copy(d).start()

    a_copy(2).wait_recv()
    pair_sum(nzy - 1, 0)

    @pl.when(m < nzy - 1)
    def _():
        z_copy(nzy - 1 - m).start()

    loop(T // CH // 2, T // CH, outputs, 0, 4)

    def x_adjoint(i, carry):
        r = blk(i, CH)
        u = XSL[window(i * CH, CH + 8), :]
        out = cvx[0:1, :] * u[:CH, :]
        for k in range(1, TAPS):
            out = out + cvx[k : k + 1, :] * pltpu.roll(u, CH + 8 - k, 0)[:CH, :]
        xg_o[r, :] = out.astype(BF16)
        return carry

    @pl.when(s < nseq - 1)
    def _():
        halo_xs.wait_recv()
        XSL[T : T + 8, :] = HSX[1]

    @pl.when(s == nseq - 1)
    def _():
        XSL[T : T + 8, :] = jnp.zeros((8, W), F32)

    loop(0, T // CH, x_adjoint, 0, 2)

    seq_wait(CXS, s_cx, r_cx)
    cx_o[...] = total(CXS, nseq)
    out = PR[m, c].astype(F32) + RA[m].astype(F32)
    for d in range(1, nzy):
        t = other_zy(d)
        send(ZS.at[t], RZ.at[t], s_z.at[d], r_z.at[t], at_zy(t)).wait_recv()
        out = out + RZ[t].astype(F32)
    bg_o[...] = out
    for d in range(1, nseq * nc):
        p, _ = other(d // 2)
        slot = p * nc + (c if d % 2 == 0 else 1 - c)
        send(CBS.at[slot], CBS.at[slot], s_cb.at[d], r_cb.at[slot], core_dev).wait_recv()
    cb_o[...] = total(CBS, nseq * nc)

    @pl.when(s < nseq - 1)
    def _():
        halo_x.wait_send()
        halo_b.wait_send()

    @pl.when(s > 0)
    def _():
        halo_bs.wait_send()
        halo_xs.wait_send()

    for d in range(1, nseq):
        state_copy(d).wait_send()
        edge_copy(d).wait_send()
        seq_copy(CXS, d, s_cx, r_cx).wait_send()
    for q in range(3):
        a_copy(q).wait_send()
    for d in range(1, nzy):
        z_copy(d).wait_send()
        cz_copy(d).wait_send()
    for d in range(1, nseq * nc):
        sc_copy(d).wait_send()


def emit(*refs):
    held, outs, sem = refs[:6], refs[6:12], refs[12]
    copies = [pltpu.make_async_copy(a, b, sem.at[i]) for i, (a, b) in enumerate(zip(held, outs))]
    for copy in copies:
        copy.start()
    for copy in copies:
        copy.wait()


def local(dims, xraw, zgate, bcraw, dt, a_rate, d_skip, conv_x, conv_bc, dout):
    nx, nyh, nz, nyl, nc = dims
    nseq = nx * nyh
    nzy = nz * nyl
    T, W = xraw.shape
    nb = T // BLOCK
    heads = W // HEAD_DIM
    N = W // 2
    own = T // (nzy * nc)
    vm = lambda *shape: pltpu.VMEM(shape[:-1], shape[-1])
    full, half = vm(T, W, F32), vm(T, W, BF16)
    ext = vm(T + 8, W, F32)
    taps = vm(TAPS, W, F32)
    dma = lambda n: pltpu.SemaphoreType.DMA((n,))
    scratch = (
        [half, half, half, vm(heads, T, F32), taps, taps, half]
        + [pltpu.SMEM((heads,), F32)] * 2
        + [ext, ext] + [full] * 7 + [ext, ext]
        + [half] * 5 + [half, vm(T, BLOCK, BF16)]
        + [vm(nb * heads, BLOCK, F32), vm(nb * heads, BLOCK, F32), vm(3 * nb * heads, BLOCK, BF16)]
        + [vm(nb, 8, W, F32)]
        + [vm(nb, N, W, F32)] * 2
        + [vm(nb, N, W, BF16)] * 2
        + [vm(2, N, W, BF16), vm(nseq, N, W, BF16)]
        + [vm(2, 16, W + N, BF16), vm(nseq, 16, W + N, BF16)]
        + [vm(nseq, N, W, F32), vm(nseq, 8, W, F32)]
        + [vm(nb, BLOCK, heads * BLOCK, BF16), vm(heads * BLOCK, W, BF16)]
        + [vm(nb, heads * BLOCK, W, BF16)]
        + [vm(16, W, BF16)] * 2 + [vm(2, 8, W, F32)] * 2
        + [vm(nzy, nc, own, W, BF16), vm(nzy, own, W, BF16)]
        + [vm(nzy, own, W, BF16)] * 2
        + [vm(nseq, TAPS, W, F32), vm(nseq * nc, TAPS, W, F32), vm(nzy, TAPS, W, F32)]
        + [dma(9)] + [dma(2)] * 2 + [dma(nseq)] * 4 + [dma(2)] * 2 + [dma(3)] * 2 + [dma(nzy)] * 2
        + [dma(nseq)] * 2 + [dma(nseq * nc)] * 2 + [dma(nzy)] * 2
    )
    vspec = pl.BlockSpec(memory_space=pltpu.VMEM)
    hspec = pl.BlockSpec(memory_space=pltpu.HBM)
    shapes = [
        ((T, W), BF16), ((T, W), BF16), ((heads, T), F32), ((own, W), F32), ((TAPS, W), F32), ((TAPS, W), F32),
    ]
    held = pl.pallas_call(
        functools.partial(kernel, dims, T, W),
        name="ssd_backward",
        out_shape=tuple(pltpu.VMEM(*sh) for sh in shapes),
        in_specs=[hspec] * 9,
        out_specs=tuple([vspec] * 6),
        scratch_shapes=scratch,
        compiler_params=pltpu.CompilerParams(
            collective_id=0, has_side_effects=True, vmem_limit_bytes=60 * 1024 * 1024
        ),
    )(xraw, zgate, bcraw, dt, a_rate, d_skip, conv_x, conv_bc, dout)
    return pl.pallas_call(
        emit,
        name="emit",
        out_shape=tuple(jax.ShapeDtypeStruct(*sh) for sh in shapes),
        in_specs=[vspec] * 6,
        out_specs=tuple([hspec] * 6),
        scratch_shapes=[dma(6)],
        compiler_params=pltpu.CompilerParams(vmem_limit_bytes=4 * 1024 * 1024),
    )(*held)


def over_mesh(torus):
    placed = (
        P(SEQ, HEAD), P(SEQ, HEAD), P(SEQ, None), P(HEAD, SEQ), P(HEAD), P(HEAD),
        P(None, HEAD), P(), P(SEQ, HEAD),
    )
    return jax.shard_map(
        functools.partial(local, tuple(torus.devices.shape)),
        mesh=torus,
        in_specs=placed,
        out_specs=(P(SEQ, HEAD), P(SEQ, HEAD), P(HEAD, SEQ), P(SEQ_HEAD, None), P(None, HEAD), P()),
        check_vma=False,
    )


def solution(mesh):
    return over_mesh(Mesh(mesh.devices.reshape(4, 2, 8, 2, 2), SEQ_HEAD))
```

```python
import functools

import jax
import jax.numpy as jnp
from jax import lax
from jax.experimental import pallas as pl
from jax.experimental.pallas import tpu as pltpu
from jax.sharding import Mesh
from jax.sharding import PartitionSpec as P

HEAD_DIM = 64
BLOCK = 256
TAPS = 4
SEQ = ("seq_0", "seq_1")
HEAD = ("head_0", "head_1", "head_2")
SEQ_HEAD = SEQ + HEAD
F32, BF16 = jnp.float32, jnp.bfloat16


def mm(a, b, dims=((1,), (0,))):
    return lax.dot_general(a, b, (dims, ((), ())), preferred_element_type=F32)


NT = ((1,), (1,))
TN = ((0,), (0,))


def parts3(v):
    p1 = v.astype(BF16)
    r1 = v - p1.astype(F32)
    p2 = r1.astype(BF16)
    r2 = r1 - p2.astype(F32)
    return p1, p2, r2.astype(BF16)


def sigmoid(v):
    return 0.5 * jnp.tanh(0.5 * v) + 0.5


def silu_slope(v):
    q = sigmoid(v)
    return q * (1.0 + v * (1.0 - q))


def loop(lo, hi, body, carry=0, unroll=1):
    if unroll >= hi - lo:
        for i in range(lo, hi):
            carry = body(i, carry)
        return carry

    def some(j, carry):
        for u in range(unroll):
            carry = body(lo + j * unroll + u, carry)
        return carry

    return lax.fori_loop(0, (hi - lo) // unroll, some, carry)


def part(k, n):
    return pl.ds(k * n if isinstance(k, int) else pl.multiple_of(k * n, n), n)


def window(start, n):
    return pl.ds(start if isinstance(start, int) else pl.multiple_of(start, 8), n)


def by_head(scalars, lanes):
    out = jnp.full(lanes.shape, scalars[3], F32)
    for h in (2, 1, 0):
        out = jnp.where(lanes == h, scalars[h], out)
    return out


def kernel(
    dims, T, W,
    xraw_h, zg_h, bcr_h, dt_h, a_h, d_h, cvx_h, cvb_h, dout_h,
    xg_o, gg_o, sg_o, bg_o, cx_o, cb_o,
    xraw, zg, bcr, dt, cvx, cvb, dout, a_s, d_s,
    XF, BCF, XS, BCS, DTE, ENT, LEA, YIN, WGIN, XSL, BS,
    XP, WX, WL, DY, DYE, BCP, MX,
    GC, DC, WP, TOT, LS, NS, SB, GB, EB, SLOT, CR, CSLOT, FS, DEC,
    KH, WXM, DYM, HXR, HBR, HSX, HSB,
    PR, RA, ZS, RZ, CXS, CBS, CBZ,
    s_in, s_h, r_h, s_st, r_st, s_cr, r_cr, s_sl, r_sl, s_a, r_a, s_z, r_z,
    s_cx, r_cx, s_cb, r_cb, s_cz, r_cz,
):
    nx, nyh, nz, nyl, nc = dims
    nseq = nx * nyh
    nzy = nz * nyl
    nb = T // BLOCK
    heads = W // HEAD_DIM
    own = T // (nzy * nc)
    sx, sy = lax.axis_index("seq_0"), lax.axis_index("seq_1")
    s = sx * nyh + sy
    z, yl, c = (lax.axis_index(n) for n in HEAD)
    m = z * nyl + yl

    def at_seq(p):
        return {"seq_0": p // nyh, "seq_1": lax.rem(p, nyh)}

    def at_zy(p):
        return {"head_0": p // nyl, "head_1": lax.rem(p, nyl)}

    def other(d):
        wrapped = (s + d) // nseq
        return s + d - nseq * wrapped, wrapped

    def other_zy(d):
        return lax.rem(m + d, nzy)

    far_first = sorted(range(1, nzy), key=lambda d: -min(d, nzy - d))

    seq_far = sorted(range(1, nseq), key=lambda d: -min(d, nseq - d))

    def send(src, dst, ss, rs, dev):
        return pltpu.make_async_remote_copy(
            src_ref=src, dst_ref=dst, send_sem=ss, recv_sem=rs,
            device_id=dev, device_id_type=pl.DeviceIdType.MESH,
        )

    core_dev = {"head_2": 1 - c}

    barrier = pltpu.get_barrier_semaphore()

    def greet(dev):
        pl.semaphore_signal(barrier, inc=1, device_id=dev, device_id_type=pl.DeviceIdType.MESH)

    for d in range(1, nseq):
        greet(at_seq(other(d)[0]))
    for d in far_first:
        greet(at_zy(other_zy(d)))
    greet(core_dev)
    for d in range(1, nseq):
        greet({**at_seq(other(d)[0]), **core_dev})

    loads = [
        pltpu.make_async_copy(a, b, s_in.at[i])
        for i, (a, b) in enumerate(
            [(dt_h, dt), (a_h, a_s), (d_h, d_s), (cvb_h, cvb), (cvx_h, cvx),
             (dout_h, dout), (zg_h, zg), (bcr_h, bcr), (xraw_h, xraw)]
        )
    ]
    for load in loads:
        load.start()

    rows16 = lax.broadcasted_iota(jnp.int32, (heads, BLOCK), 0)
    n16 = nb * heads
    ri = lax.broadcasted_iota(jnp.int32, (BLOCK, BLOCK), 0)
    ci = lax.broadcasted_iota(jnp.int32, (BLOCK, BLOCK), 1)
    tri = (ri <= ci).astype(F32).astype(BF16)
    rr = lax.rem(lax.broadcasted_iota(jnp.int32, (3 * n16, W), 0), n16)
    ll = lax.broadcasted_iota(jnp.int32, (3 * n16, W), 1) // HEAD_DIM
    for load in loads[:3]:
        load.wait()
    a_col = by_head([a_s[h] for h in range(heads)], rows16)
    for k in range(nb):
        piece = dt[:, k * BLOCK : (k + 1) * BLOCK]
        DC[k * heads : (k + 1) * heads, :] = piece
        GC[k * heads : (k + 1) * heads, :] = piece * a_col
    w3 = mm(jnp.concatenate(parts3(GC[...]), axis=0), tri)
    within = w3[:n16] + w3[n16 : 2 * n16] + w3[2 * n16 :]
    GC[...] = within
    wp = jnp.concatenate(parts3(within), axis=0)
    dp = jnp.concatenate(parts3(DC[...]), axis=0)
    WP[...] = wp

    def blk(k, n=BLOCK):
        return part(k, n)

    def expand(k, carry):
        hot = ((rr // heads == k) & (lax.rem(rr, heads) == ll)).astype(F32).astype(BF16)
        wexp = mm(wp, hot, TN)
        total = wexp[BLOCK - 1 : BLOCK, :]
        TOT[k] = jnp.broadcast_to(total, (8, W))
        ENT[blk(k), :] = jnp.exp(-wexp)
        LEA[blk(k), :] = jnp.exp(jnp.minimum(wexp - total, 0.0))
        DTE[blk(k), :] = mm(dp, hot, TN)
        return carry

    loop(0, nb, expand, 0, 2)

    CH = 64
    N = W // 2
    per = BLOCK // CH
    for load in loads[3:8]:
        load.wait()
    XF[0:8, :] = jnp.zeros((8, W), F32)
    BCF[0:8, :] = jnp.zeros((8, W), F32)

    def gates(i, carry):
        r = blk(i, CH)
        zv = zg[r, :].astype(F32)
        dy = (dout[r, :].astype(F32) * (zv * sigmoid(zv))).astype(BF16)
        DY[r, :] = dy
        DYE[r, :] = (dy.astype(F32) * ENT[r, :]).astype(BF16)
        shifted = window(8 + i * CH, CH)
        BCF[shifted, :] = bcr[r, :].astype(F32)
        return carry

    loop(0, T // CH, gates, 0, 2)

    def pre(F, taps, i):
        v = F[window(i * CH, CH + 8), :]
        out = taps[0:1, :] * v[8:, :]
        for k in range(1, TAPS):
            out = out + taps[k : k + 1, :] * pltpu.roll(v, k, 0)[8:, :]
        return out

    def conv_bc_chunk(i, carry):
        v = pre(BCF, cvb, i)
        BCP[blk(i, CH), :] = (v * sigmoid(v)).astype(BF16)
        BCS[blk(i, CH), :] = v
        return carry

    def conv_x_chunk(i, carry):
        r = blk(i, CH)
        v = pre(XF, cvx, i)
        post = (v * sigmoid(v)).astype(BF16)
        XP[r, :] = post
        XS[r, :] = v
        wx = (post.astype(F32) * DTE[r, :]).astype(BF16)
        WX[r, :] = wx
        WL[r, :] = (wx.astype(F32) * LEA[r, :]).astype(BF16)
        return carry

    loop(0, T // CH, conv_bc_chunk, 0, 2)
    rt = lax.broadcasted_iota(jnp.int32, (16, W), 0)
    edge = rt < TAPS - 1
    BCP[0:16, :] = jnp.where(edge, jnp.zeros((16, W), BF16), BCP[0:16, :])

    grads = [mm(BCP[blk(k), N:], DYE[blk(k), :], TN) for k in range(nb)]
    grad = jnp.zeros((N, W), F32)
    for k in reversed(range(nb)):
        NS[k] = grad
        grad = jnp.exp(-TOT[k][0:1, :]) * grad + grads[k]
    EB[1] = grad.astype(BF16)

    pl.semaphore_wait(barrier, nseq * nc - 1 + nzy - 1)

    loads[8].wait()
    halo_x = send(xraw.at[T - 16 :], HXR, s_h.at[0], r_h.at[0], at_seq(s + 1))
    halo_b = send(bcr.at[T - 16 :], HBR, s_h.at[1], r_h.at[1], at_seq(s + 1))

    @pl.when(s < nseq - 1)
    def _():
        halo_x.start()
        halo_b.start()

    def state_copy(d):
        p, wrapped = other(d)
        return send(EB.at[wrapped], SLOT.at[s], s_st.at[d], r_st.at[s], at_seq(p))

    def edge_copy(d):
        p, wrapped = other(d)
        return send(CR.at[wrapped], CSLOT.at[s], s_cr.at[d], r_cr.at[s], at_seq(p))

    for d in seq_far:

        @pl.when(s + d >= nseq)
        def _():
            state_copy(d).start()

    def widen(i, carry):
        XF[window(8 + i * CH, CH), :] = xraw[blk(i, CH), :].astype(F32)
        return conv_x_chunk(i, carry)

    loop(0, T // CH, widen, 0, 2)
    ends = [mm(BCP[blk(k), :N], WL[blk(k), :], TN) for k in range(nb)]
    state = jnp.zeros((N, W), F32)
    for k in range(nb):
        LS[k] = state
        state = jnp.exp(-TOT[k][0:1, :]) * state + ends[k]
    EB[0] = state.astype(BF16)
    for d in seq_far:

        @pl.when(s + d < nseq)
        def _():
            state_copy(d).start()

    lane_h = lax.broadcasted_iota(jnp.int32, (BLOCK, W), 1) // HEAD_DIM
    r512 = lax.rem(lax.broadcasted_iota(jnp.int32, (3 * n16, heads * 128), 0), n16)
    l512 = lax.broadcasted_iota(jnp.int32, (3 * n16, heads * 128), 1) // 128
    for h in range(heads):
        KH[:, 0:128, h * BLOCK + 128 : (h + 1) * BLOCK] = jnp.zeros((nb, 128, 128), BF16)
    TQ = 64

    def inside(k, carry):
        bm, cm = BCP[blk(k), :N], BCP[blk(k), N:]
        wx, dy = WX[blk(k), :], DY[blk(k), :]
        for h in range(heads):
            DYM[k, h * BLOCK : (h + 1) * BLOCK, :] = jnp.where(lane_h == h, dy, jnp.zeros_like(dy))
        hot = ((r512 // heads == k) & (lax.rem(r512, heads) == l512)).astype(F32).astype(BF16)
        col = mm(WP[...], hot, TN)
        for t0 in range(0, BLOCK, TQ):
            ext = 128 if t0 < 128 else BLOCK
            sc = mm(cm[t0 : t0 + TQ, :], bm[0:ext, :], NT)
            tt = t0 + lax.broadcasted_iota(jnp.int32, (TQ, ext), 0)
            ss = lax.broadcasted_iota(jnp.int32, (TQ, ext), 1)
            keep = tt >= ss
            total = None
            for h in range(heads):
                wrow = GC[pl.ds(k * heads + h, 1), :][:, 0:ext]
                wcol = col[t0 : t0 + TQ, h * 128 : (h + 1) * 128]
                if ext > 128:
                    wcol = jnp.concatenate([wcol, wcol], axis=1)
                decay = jnp.where(keep, jnp.exp(jnp.minimum(wrow - wcol, 0.0)), 0.0)
                KH[k, t0 : t0 + TQ, h * BLOCK : h * BLOCK + ext] = (sc * decay).astype(BF16)
                mixing = mm(DYM[k, h * BLOCK + t0 : h * BLOCK + t0 + TQ, :], wx[0:ext, :], NT)
                part = mixing * decay
                total = part if total is None else total + part
            rows = window(k * BLOCK + t0, TQ)
            MX[rows, 0:ext] = total.astype(BF16)
            if ext < BLOCK:
                MX[rows, ext:] = jnp.zeros((TQ, BLOCK - ext), BF16)
        return carry

    def inner(k, carry):
        wx = WX[blk(k), :]
        for h in range(heads):
            WXM[h * BLOCK : (h + 1) * BLOCK, :] = jnp.where(lane_h == h, wx, jnp.zeros_like(wx))
        acc = None
        for h in range(heads):
            part_h = mm(
                KH[k, :, h * BLOCK : (h + 1) * BLOCK], DYM[k, h * BLOCK : (h + 1) * BLOCK, :], TN
            )
            acc = part_h if acc is None else acc + part_h
        WGIN[blk(k), :] = acc
        YIN[blk(k), :] = mm(KH[k], WXM[...])
        return carry

    loop(nb - 1, nb, inside, 0, 1)

    @pl.when(s > 0)
    def _():
        halo_x.wait_recv()
        halo_b.wait_recv()
        XF[0:8, :] = HXR[8:16, :].astype(F32)
        BCF[0:8, :] = HBR[8:16, :].astype(F32)

    conv_bc_chunk(0, 0)
    conv_x_chunk(0, 0)
    dtot = TOT[0][0:1, :]
    for k in range(1, nb):
        dtot = dtot + TOT[k][0:1, :]
    tail0 = TOT[0][0:1, :]
    q1, q2, q3 = (p.astype(F32) for p in parts3(dtot))

    def edge_rows(v):
        v = jnp.where(edge, v, 0.0)
        v = jnp.where(rt == 8, q1, jnp.where(rt == 9, q2, jnp.where(rt == 10, q3, v)))
        return v.astype(BF16)

    CR[0, :, 0:W] = edge_rows(
        WX[0:16, :].astype(F32) * LEA[0:16, :] * jnp.exp(jnp.minimum(tail0 - dtot, 0.0))
    )
    CR[1, :, 0:W] = edge_rows(DYE[0:16, :].astype(F32))
    first = jnp.where(edge, BCP[0:16, :], jnp.zeros((16, W), BF16))
    CR[0, :, W:] = first[:, :N]
    CR[1, :, W:] = first[:, N:]
    for d in seq_far:
        edge_copy(d).start()
    start0 = mm(first[:, :N], WL[0:16, :], TN)

    loop(0, nb - 1, inside, 0, 1)

    def mixed(k, carry):
        r = blk(k)
        mx = MX[r, :]
        BS[r, :N] = mm(mx, BCP[r, N:], TN)
        BS[r, N:] = mm(mx, BCP[r, :N])
        BCS[r, :] = silu_slope(BCS[r, :])
        return carry

    loop(0, nb, mixed, 0, 4)

    for d in range(1, nseq):
        p, _ = other(d)
        send(EB.at[0], SLOT.at[p], s_st.at[d], r_st.at[p], at_seq(p)).wait_recv()
        send(CR.at[0], CSLOT.at[p], s_cr.at[d], r_cr.at[p], at_seq(p)).wait_recv()

    for d in range(1, nseq):
        p, _ = other(d)
        rows = CSLOT[p, :, 0:W]
        t3 = rows[8:16, :].astype(F32)
        DEC[p] = jnp.broadcast_to(jnp.exp(-(t3[0:1, :] + t3[1:2, :] + t3[2:3, :])), (8, W))
        FS[p] = SLOT[p].astype(F32) + mm(CSLOT[p, :, W:], rows, TN)

    def fold(p, value):
        return DEC[p][0:1, :] * value + FS[p]

    zero_state = jnp.zeros((N, W), F32)
    s_first = lax.fori_loop(0, s, fold, zero_state)
    g_last = lax.fori_loop(0, nseq - 1 - s, lambda i, v: fold(nseq - 1 - i, v), zero_state)
    SB[0] = s_first.astype(BF16)
    s_next = jnp.exp(-TOT[0][0:1, :]) * s_first + start0
    before = jnp.zeros((1, W), F32)
    for k in range(1, nb):
        SB[k] = (LS[k] + jnp.exp(-before) * s_next).astype(BF16)
        before = before + TOT[k][0:1, :]
    after = jnp.zeros((1, W), F32)
    for k in reversed(range(nb)):
        GB[k] = (NS[k] + jnp.exp(-after) * g_last).astype(BF16)
        after = after + TOT[k][0:1, :]

    def shared(k, carry):
        r = blk(k)
        BS[r, :N] = (BS[r, :N] + mm(WL[r, :], GB[k], NT)) * BCS[r, :N]
        BS[r, N:] = (BS[r, N:] + mm(DYE[r, :], SB[k], NT)) * BCS[r, N:]
        return carry

    shared(0, 0)
    HSB[0] = BS[0:8, :]
    halo_bs = send(HSB.at[0], HSB.at[1], s_sl.at[0], r_sl.at[0], at_seq(s - 1))

    @pl.when(s > 0)
    def _():
        halo_bs.start()

    loop(1, nb, shared, 0, 3)

    def bc_adjoint(j, carry):
        u = BS[window(j * own, own + 8), :]
        out = cvb[0:1, :] * u[:own, :]
        for k in range(1, TAPS):
            out = out + cvb[k : k + 1, :] * pltpu.roll(u, own + 8 - k, 0)[:own, :]
        PR[j // nc, lax.rem(j, nc)] = out.astype(BF16)
        return carry

    pieces = [(0, nzy // 2), (nzy // 2, nzy - 1), (nzy - 1, nzy)]

    def a_copy(q):
        lo, hi = pieces[q]
        part = pl.ds(lo, hi - lo)
        return send(PR.at[part, 1 - c], RA.at[part], s_a.at[q], r_a.at[q], core_dev)

    def adjoint_piece(q):
        loop(pieces[q][0] * nc, pieces[q][1] * nc, bc_adjoint, 0, 2)
        a_copy(q).start()

    def pair_sum(i, carry):
        ZS[i] = (PR[i, c].astype(F32) + RA[i].astype(F32)).astype(BF16)
        return carry

    def z_copy(d):
        t = other_zy(d)
        return send(ZS.at[t], RZ.at[m], s_z.at[d], r_z.at[m], at_zy(t))

    def tap_sums(slope, F, start, carry):
        n = slope.shape[0]
        v = F[window(start, n + 8), :]
        out = []
        for k in range(TAPS):
            moved = v[8:, :] if k == 0 else pltpu.roll(v, k, 0)[8:, :]
            out.append(carry[k] + (slope * moved).reshape(n // 8, 8, W).sum(axis=0))
        return tuple(out)

    def stack_taps(sums):
        rt4 = lax.broadcasted_iota(jnp.int32, (TAPS, W), 0)
        out = jnp.zeros((TAPS, W), F32)
        for k in range(TAPS):
            out = jnp.where(rt4 == k, jnp.sum(sums[k], axis=0, keepdims=True), out)
        return out

    zero4 = tuple(jnp.zeros((8, W), F32) for _ in range(TAPS))
    sums = loop(
        0, T // CH, lambda i, cr: tap_sums(BS[blk(i, CH), :], BCF, i * CH, cr), zero4, 2
    )
    CBZ[m] = stack_taps(sums)

    def cz_copy(d):
        return send(CBZ.at[m], CBZ.at[m], s_cz.at[d], r_cz.at[m], at_zy(other_zy(d)))

    for d in far_first:
        cz_copy(d).start()

    adjoint_piece(0)
    adjoint_piece(1)

    def seq_copy(buf, d, ss, rs):
        p, _ = other(d)
        return send(buf.at[s], buf.at[s], ss.at[d], rs.at[s], at_seq(p))

    def seq_wait(buf, ss, rs):
        for d in range(1, nseq):
            p, _ = other(d)
            send(buf.at[p], buf.at[p], ss.at[d], rs.at[p], at_seq(p)).wait_recv()

    CW = 128
    lane1 = lax.broadcasted_iota(jnp.int32, (1, W), 1) // HEAD_DIM
    skip = by_head([d_s[h] for h in range(heads)], lane1)
    pick = (
        lax.broadcasted_iota(jnp.int32, (16, W), 0)
        == lax.broadcasted_iota(jnp.int32, (16, W), 1) // HEAD_DIM
    ).astype(F32).astype(BF16)

    def channels(i, carry):
        r = blk(i, CW)
        k = i // (BLOCK // CW)
        wg = WGIN[r, :] + LEA[r, :] * mm(BCP[r, :N], GB[k])
        xp = XP[r, :].astype(F32)
        slope = (DTE[r, :] * wg + skip * DY[r, :].astype(F32)) * silu_slope(XS[r, :])
        XSL[r, :] = slope
        prod = xp * wg
        hi = prod.astype(BF16)
        lo = (prod - hi.astype(F32)).astype(BF16)
        steps = mm(pick, hi, NT) + mm(pick, lo, NT)
        sg_o[:, part(i, CW)] = steps[0:heads, :]
        return tap_sums(slope, XF, i * CW, carry)

    halves = BLOCK // CW

    def block_channels(k, sums):
        inner(k, 0)
        return loop(k * halves, (k + 1) * halves, channels, sums, halves)

    sums = block_channels(0, zero4)
    HSX[0] = XSL[0:8, :]
    halo_xs = send(HSX.at[0], HSX.at[1], s_sl.at[1], r_sl.at[1], at_seq(s - 1))

    @pl.when(s > 0)
    def _():
        halo_xs.start()

    for q in range(2):
        a_copy(q).wait_recv()
        loop(pieces[q][0], pieces[q][1], pair_sum, 0, nzy)
    for d in far_first:

        @pl.when(other_zy(d) < nzy - 1)
        def _():
            z_copy(d).start()

    sums = block_channels(1, sums)
    sums = block_channels(2, sums)
    sums = block_channels(3, sums)
    CXS[s] = stack_taps(sums)
    for d in range(1, nseq):
        seq_copy(CXS, d, s_cx, r_cx).start()

    def total(buf, n):
        out = buf[0]
        for p in range(1, n):
            out = out + buf[p]
        return out

    def outputs(i, carry):
        r = blk(i, CH)
        k = i // (BLOCK // CH)
        y = YIN[r, :] + ENT[r, :] * mm(BCP[r, N:], SB[k]) + skip * XP[r, :].astype(F32)
        gate = dout[r, :].astype(F32) * silu_slope(zg[r, :].astype(F32))
        gg_o[r, :] = (gate * y).astype(BF16)
        return carry

    @pl.when(s < nseq - 1)
    def _():
        halo_bs.wait_recv()
        BS[T : T + 8, :] = HSB[1]

    @pl.when(s == nseq - 1)
    def _():
        BS[T : T + 8, :] = jnp.zeros((8, W), F32)

    adjoint_piece(2)
    loop(0, T // CH // 2, outputs, 0, 4)
    for d in range(1, nzy):
        t = other_zy(d)
        send(CBZ.at[t], CBZ.at[t], s_cz.at[d], r_cz.at[t], at_zy(t)).wait_recv()
    mine = s * nc + c
    CBS[mine] = total(CBZ, nzy)

    def sc_copy(d):
        p, _ = other(d // 2)
        dev = at_seq(p) if d % 2 == 0 else {**at_seq(p), **core_dev}
        return send(CBS.at[mine], CBS.at[mine], s_cb.at[d], r_cb.at[mine], dev)

    for d in seq_far:
        sc_copy(2 * d + 1).start()
        sc_copy(2 * d).start()
    sc_copy(1).start()

    a_copy(2).wait_recv()
    pair_sum(nzy - 1, 0)

    @pl.when(m < nzy - 1)
    def _():
        z_copy(nzy - 1 - m).start()

    loop(T // CH // 2, T // CH, outputs, 0, 4)

    def x_adjoint(i, carry):
        r = blk(i, CH)
        u = XSL[window(i * CH, CH + 8), :]
        out = cvx[0:1, :] * u[:CH, :]
        for k in range(1, TAPS):
            out = out + cvx[k : k + 1, :] * pltpu.roll(u, CH + 8 - k, 0)[:CH, :]
        xg_o[r, :] = out.astype(BF16)
        return carry

    @pl.when(s < nseq - 1)
    def _():
        halo_xs.wait_recv()
        XSL[T : T + 8, :] = HSX[1]

    @pl.when(s == nseq - 1)
    def _():
        XSL[T : T + 8, :] = jnp.zeros((8, W), F32)

    loop(0, T // CH, x_adjoint, 0, 2)

    seq_wait(CXS, s_cx, r_cx)
    cx_o[...] = total(CXS, nseq)
    out = PR[m, c].astype(F32) + RA[m].astype(F32)
    for d in range(1, nzy):
        t = other_zy(d)
        send(ZS.at[t], RZ.at[t], s_z.at[d], r_z.at[t], at_zy(t)).wait_recv()
        out = out + RZ[t].astype(F32)
    bg_o[...] = out
    for d in range(1, nseq * nc):
        p, _ = other(d // 2)
        slot = p * nc + (c if d % 2 == 0 else 1 - c)
        send(CBS.at[slot], CBS.at[slot], s_cb.at[d], r_cb.at[slot], core_dev).wait_recv()
    cb_o[...] = total(CBS, nseq * nc)

    @pl.when(s < nseq - 1)
    def _():
        halo_x.wait_send()
        halo_b.wait_send()

    @pl.when(s > 0)
    def _():
        halo_bs.wait_send()
        halo_xs.wait_send()

    for d in range(1, nseq):
        state_copy(d).wait_send()
        edge_copy(d).wait_send()
        seq_copy(CXS, d, s_cx, r_cx).wait_send()
    for q in range(3):
        a_copy(q).wait_send()
    for d in range(1, nzy):
        z_copy(d).wait_send()
        cz_copy(d).wait_send()
    for d in range(1, nseq * nc):
        sc_copy(d).wait_send()


def emit(*refs):
    held, outs, sem = refs[:6], refs[6:12], refs[12]
    copies = [pltpu.make_async_copy(a, b, sem.at[i]) for i, (a, b) in enumerate(zip(held, outs))]
    for copy in copies:
        copy.start()
    for copy in copies:
        copy.wait()


def local(dims, xraw, zgate, bcraw, dt, a_rate, d_skip, conv_x, conv_bc, dout):
    nx, nyh, nz, nyl, nc = dims
    nseq = nx * nyh
    nzy = nz * nyl
    T, W = xraw.shape
    nb = T // BLOCK
    heads = W // HEAD_DIM
    N = W // 2
    own = T // (nzy * nc)
    vm = lambda *shape: pltpu.VMEM(shape[:-1], shape[-1])
    full, half = vm(T, W, F32), vm(T, W, BF16)
    ext = vm(T + 8, W, F32)
    taps = vm(TAPS, W, F32)
    dma = lambda n: pltpu.SemaphoreType.DMA((n,))
    scratch = (
        [half, half, half, vm(heads, T, F32), taps, taps, half]
        + [pltpu.SMEM((heads,), F32)] * 2
        + [ext, ext] + [full] * 7 + [ext, ext]
        + [half] * 5 + [half, vm(T, BLOCK, BF16)]
        + [vm(nb * heads, BLOCK, F32), vm(nb * heads, BLOCK, F32), vm(3 * nb * heads, BLOCK, BF16)]
        + [vm(nb, 8, W, F32)]
        + [vm(nb, N, W, F32)] * 2
        + [vm(nb, N, W, BF16)] * 2
        + [vm(2, N, W, BF16), vm(nseq, N, W, BF16)]
        + [vm(2, 16, W + N, BF16), vm(nseq, 16, W + N, BF16)]
        + [vm(nseq, N, W, F32), vm(nseq, 8, W, F32)]
        + [vm(nb, BLOCK, heads * BLOCK, BF16), vm(heads * BLOCK, W, BF16)]
        + [vm(nb, heads * BLOCK, W, BF16)]
        + [vm(16, W, BF16)] * 2 + [vm(2, 8, W, F32)] * 2
        + [vm(nzy, nc, own, W, BF16), vm(nzy, own, W, BF16)]
        + [vm(nzy, own, W, BF16)] * 2
        + [vm(nseq, TAPS, W, F32), vm(nseq * nc, TAPS, W, F32), vm(nzy, TAPS, W, F32)]
        + [dma(9)] + [dma(2)] * 2 + [dma(nseq)] * 4 + [dma(2)] * 2 + [dma(3)] * 2 + [dma(nzy)] * 2
        + [dma(nseq)] * 2 + [dma(nseq * nc)] * 2 + [dma(nzy)] * 2
    )
    vspec = pl.BlockSpec(memory_space=pltpu.VMEM)
    hspec = pl.BlockSpec(memory_space=pltpu.HBM)
    shapes = [
        ((T, W), BF16), ((T, W), BF16), ((heads, T), F32), ((own, W), F32), ((TAPS, W), F32), ((TAPS, W), F32),
    ]
    held = pl.pallas_call(
        functools.partial(kernel, dims, T, W),
        name="ssd_backward",
        out_shape=tuple(pltpu.VMEM(*sh) for sh in shapes),
        in_specs=[hspec] * 9,
        out_specs=tuple([vspec] * 6),
        scratch_shapes=scratch,
        compiler_params=pltpu.CompilerParams(
            collective_id=0, has_side_effects=True, vmem_limit_bytes=60 * 1024 * 1024
        ),
    )(xraw, zgate, bcraw, dt, a_rate, d_skip, conv_x, conv_bc, dout)
    return pl.pallas_call(
        emit,
        name="emit",
        out_shape=tuple(jax.ShapeDtypeStruct(*sh) for sh in shapes),
        in_specs=[vspec] * 6,
        out_specs=tuple([hspec] * 6),
        scratch_shapes=[dma(6)],
        compiler_params=pltpu.CompilerParams(vmem_limit_bytes=4 * 1024 * 1024),
    )(*held)


def over_mesh(torus):
    placed = (
        P(SEQ, HEAD), P(SEQ, HEAD), P(SEQ, None), P(HEAD, SEQ), P(HEAD), P(HEAD),
        P(None, HEAD), P(), P(SEQ, HEAD),
    )
    return jax.shard_map(
        functools.partial(local, tuple(torus.devices.shape)),
        mesh=torus,
        in_specs=placed,
        out_specs=(P(SEQ, HEAD), P(SEQ, HEAD), P(HEAD, SEQ), P(SEQ_HEAD, None), P(None, HEAD), P()),
        check_vma=False,
    )


def solution(mesh):
    return over_mesh(Mesh(mesh.devices.reshape(4, 2, 8, 2, 2), SEQ_HEAD))
```
